32 devices in a mesh: gx: 4 (over z), gy: 2 (over x), gz: 4 (over y, core).
Axes of the slice: x: 2, y: 2, z: 4, core: 2. Of those that a mesh axis runs over, the one named last changes fastest.
Arguments:
- right_side: float32 [4, 2, 8, 128], P('gx', 'gy', 'gz'), may hold values from -8 to 8
- diag_blocks: float32 [4, 2, 8, 128, 128], P('gx', 'gy', 'gz'), may hold values from -0.035 to 2.04, as said below
- couplings: float32 [3, 4, 2, 8, 128, 128], P(None, 'gx', 'gy', 'gz'), may hold values from -0.04 to 0.04
- pattern: int32 [3, 4, 2, 8], P(None, 'gx', 'gy', 'gz'), may hold values 0 or 1
- deflation: float32 [4, 2, 8, 32, 128], P('gx', 'gy', 'gz'), may hold values from -5 to 5
Outputs:
- solution: float32 [4, 2, 8, 128], P('gx', 'gy', 'gz')
- residual: float32 [4, 2, 8, 128], P('gx', 'gy', 'gz')
The draws below stay inside these ranges and needn't reach their ends.
Inputs may be any that keep to these rules, and one draw needn't show every extreme that they name: `diag_blocks`: each diagonal block is symmetric.
All inputs are finite; a program needn't handle non-finite values. No bound on the sum of `pattern` on one device may be relied on, other than what follows from the above.
Results may differ from the reference program's by a relative error of at most 0.00035.
Values sent between devices are 32-bit elements; how exact they have to be, the bound alone decides.
A program may use at most 64 MiB of HBM per device.

```python
import math
import jax
import jax.numpy as jnp
from jax import lax

BLOCK = 128
DEFL = 32
ITERS = 3
NBX = 4
NBY = 2
NBZ = 8


def deflation_basis(key):
    drawn = jax.random.normal(jax.random.fold_in(key, 101), (NBX, NBY, NBZ, DEFL, BLOCK), jnp.float32)
    return jnp.clip(drawn, -5.0, 5.0)


def draw_deflation(key, part):
    return deflation_basis(key)


def draw_right_side(key, part):
    basis = deflation_basis(key)
    mixing = jnp.clip(jax.random.normal(jax.random.fold_in(key, 102), (DEFL,), jnp.float32), -4.0, 4.0) * 0.25
    extent_all = (NBX, NBY, NBZ, BLOCK)
    jitter = jnp.clip(jax.random.normal(jax.random.fold_in(key, 103), extent_all, jnp.float32), -4.0, 4.0)
    combined = jitter + jnp.einsum('a,xyzak->xyzk', mixing, basis)
    return jnp.clip(combined, -8.0, 8.0)


def draw_diag_blocks(key, part):
    extent_all = (NBX, NBY, NBZ, BLOCK, BLOCK)
    jitter = jnp.clip(jax.random.normal(jax.random.fold_in(key, 201), extent_all, jnp.float32) * 0.006, -0.024, 0.024)
    mirrored = (jitter + jnp.swapaxes(jitter, -1, -2)) * 0.7071
    levels = jnp.exp(jax.random.uniform(jax.random.fold_in(key, 202), (NBX, NBY, NBZ, BLOCK), jnp.float32, 0.0, math.log(2.0)))
    identity = jnp.eye(BLOCK, dtype=jnp.float32)
    return mirrored + levels[..., None] * identity


def draw_couplings(key, part):
    extent_all = (3, NBX, NBY, NBZ, BLOCK, BLOCK)
    return jnp.clip(jax.random.normal(jax.random.fold_in(key, 301), extent_all, jnp.float32) * 0.01, -0.04, 0.04)


def touch_ends(entries, own_key, least, largest):
    index_at = [jax.random.randint(jax.random.fold_in(own_key, axis), (), 0, length) for axis, length in enumerate(entries.shape)]
    widest = entries.shape.index(max(entries.shape))
    next_to = index_at[:widest] + [(index_at[widest] + 1) % entries.shape[widest]] + index_at[widest + 1:]
    return entries.at[tuple(index_at)].set(least).at[tuple(next_to)].set(largest)


def setup_inputs(seed: int = 0) -> dict:
    arg_keys = jax.random.split(jax.random.key(seed), 6)
    return {
        "right_side": draw_right_side(jax.random.fold_in(arg_keys[5], 71), 0),
        "diag_blocks": draw_diag_blocks(jax.random.fold_in(arg_keys[5], 71), 0),
        "couplings": draw_couplings(jax.random.fold_in(arg_keys[5], 71), 0),
        "pattern": touch_ends((jax.random.randint(arg_keys[3], (3, NBX, NBY, NBZ), 0, 4) < 3).astype(jnp.int32), jax.random.fold_in(arg_keys[3], 1), 0, 1),
        "deflation": draw_deflation(jax.random.fold_in(arg_keys[5], 71), 0),
    }


HIGHEST = lax.Precision.HIGHEST

def rows_times(blocks, vectors):
    return jnp.einsum('xyzrk,xyzck->xyzcr', blocks, vectors, precision=HIGHEST)

def cols_times(blocks, vectors):
    return jnp.einsum('xyzkr,xyzck->xyzcr', blocks, vectors, precision=HIGHEST)

def toward_low(vectors, axis_num):
    extent = vectors.shape[axis_num]
    upper = lax.slice_in_dim(vectors, 1, extent, axis=axis_num)
    zeros_face = jnp.zeros_like(lax.slice_in_dim(vectors, 0, 1, axis=axis_num))
    return jnp.concatenate([upper, zeros_face], axis=axis_num)

def toward_high(vectors, axis_num):
    extent = vectors.shape[axis_num]
    lower = lax.slice_in_dim(vectors, 0, extent - 1, axis=axis_num)
    zeros_face = jnp.zeros_like(lax.slice_in_dim(vectors, 0, 1, axis=axis_num))
    return jnp.concatenate([zeros_face, lower], axis=axis_num)

def operate(diag_blocks, couplings, weights, vectors):
    accum_sum = rows_times(diag_blocks, vectors)
    for axis_num in range(3):
        coupled = couplings[axis_num]
        gate_w = weights[axis_num][:, :, :, None, None]
        accum_sum = accum_sum + gate_w * rows_times(coupled, toward_low(vectors, axis_num))
        accum_sum = accum_sum + toward_high(gate_w * cols_times(coupled, vectors), axis_num)
    return accum_sum

def spread(coarse_coef, basis):
    return jnp.einsum('a,xyzak->xyzk', coarse_coef, basis, precision=HIGHEST)

def reference(right_side, diag_blocks, couplings, pattern, deflation):
    weights = pattern.astype(jnp.float32)
    applied = operate(diag_blocks, couplings, weights, deflation)
    coarse_mat = jnp.einsum('xyzak,xyzbk->ab', deflation, applied, precision=HIGHEST)
    coarse_mat = 0.5 * (coarse_mat + coarse_mat.T)
    factor = jnp.linalg.cholesky(coarse_mat)
    projected = jnp.einsum('xyzak,xyzk->a', deflation, right_side, precision=HIGHEST)
    coarse_coef = jax.scipy.linalg.cho_solve((factor, True), projected)
    solution = spread(coarse_coef, deflation)
    residual = right_side - spread(coarse_coef, applied)
    norm_sq = jnp.sum(residual * residual)
    projected = jnp.einsum('xyzak,xyzk->a', applied, residual, precision=HIGHEST)
    coarse_coef = jax.scipy.linalg.cho_solve((factor, True), projected)
    direction = residual - spread(coarse_coef, deflation)
    for iteration in range(ITERS):
        images = operate(diag_blocks, couplings, weights, direction[:, :, :, None, :])[:, :, :, 0, :]
        step_len = norm_sq / jnp.sum(direction * images)
        solution = solution + step_len * direction
        residual = residual - step_len * images
        if iteration + 1 < ITERS:
            norm_new = jnp.sum(residual * residual)
            projected = jnp.einsum('xyzak,xyzk->a', applied, residual, precision=HIGHEST)
            coarse_coef = jax.scipy.linalg.cho_solve((factor, True), projected)
            direction = residual + norm_new / norm_sq * direction - spread(coarse_coef, deflation)
            norm_sq = norm_new
    return (solution, residual)
```

```python
import functools
import math

import jax
import jax.numpy as jnp
from jax import lax
from jax.experimental import pallas as pl
from jax.experimental.pallas import tpu as pltpu
from jax.sharding import PartitionSpec as P

ITERS = 3
AXES = ("gx", "gy", "gz")
COARSE_GROUPS = (("gy", "gz"), ("gx",))
UNROLLED = 32
LAST_GROUPS = (("gx", "gy", "gz"),)
DIRECT = 64
SHIFT = 1.45
GJ_FIRST = 10
MESH = pl.DeviceIdType.MESH
F32 = jnp.float32
BF16 = jnp.bfloat16


def place(index, group, sizes):
    coords = {}
    for axis in reversed(group):
        coords[axis] = lax.rem(index, sizes[axis])
        index = lax.div(index, sizes[axis])
    return coords


def position(group, sizes):
    index = 0
    for axis in group:
        index = index * sizes[axis] + lax.axis_index(axis)
    return index


def extent(group, sizes):
    return math.prod(sizes[axis] for axis in group)


def for_peers(group, sizes, action):
    count = extent(group, sizes)
    me = position(group, sizes)

    def body(k, carry):
        action(place(lax.rem(me + k, count), group, sizes))
        return carry

    if count <= UNROLLED:
        for k in range(1, count):
            body(k, 0)
    else:
        lax.fori_loop(1, count, body, 0)


def split_rows(v):
    high = v.astype(BF16).astype(F32)
    rest = v - high
    middle = rest.astype(BF16).astype(F32)
    low = rest - middle
    return jnp.concatenate([high, middle, low], axis=0).astype(BF16)


def join_rows(out, rows):
    return out[:rows] + (out[rows : 2 * rows] + out[2 * rows : 3 * rows])


def split_pair(m):
    high = m.astype(BF16)
    return high, (m - high.astype(F32)).astype(BF16)


def times(parts, high, low):
    out = jnp.dot(parts, high, preferred_element_type=F32)
    out = out + jnp.dot(parts, low, preferred_element_type=F32)
    return join_rows(out, parts.shape[0] // 3)


def times_t(parts, high, low):
    dims = (((1,), (1,)), ((), ()))
    out = lax.dot_general(parts, high, dims, preferred_element_type=F32)
    out = out + lax.dot_general(parts, low, dims, preferred_element_type=F32)
    return join_rows(out, parts.shape[0] // 3)


def last_groups(sizes):
    return LAST_GROUPS if extent(LAST_GROUPS[0], sizes) <= DIRECT else COARSE_GROUPS


def kernel(sizes, lz, block, defl, *refs):
    inputs = refs[:5]
    sol_ref, res_ref = refs[5:7]
    (loc_h, loc_l, out_h, out_l, in_h, in_l, zo_h, zo_l, zi_h, zi_l, proj_h, proj_l) = refs[7:19]
    n_ops = 1 + ITERS
    at = 19
    ops = []
    for _ in range(n_ops):
        ops.append(refs[at : at + 10])
        at += 10
    stages = len(COARSE_GROUPS)
    moment_bufs = [refs[at + j * stages : at + (j + 1) * stages] for j in range(ITERS)]
    at += ITERS * stages
    final_groups = last_groups(sizes)
    final_bufs = refs[at : at + len(final_groups)]
    at += len(final_groups)
    halo_send, halo_recv, red_send, red_recv, load_sem = refs[at : at + 5]
    staged = refs[at + 5 : at + 10]
    loads = [pltpu.make_async_copy(src, dst, load_sem.at[k]) for k, (src, dst) in enumerate(zip(inputs, staged))]
    for k in (0, 4, 3, 2, 1):
        loads[k].start()
    right_ref, diag_ref, coup_ref, pat_ref, defl_ref = staged

    idx = {axis: lax.axis_index(axis) for axis in AXES}
    lower = {axis: idx[axis] > 0 for axis in AXES}
    upper = {axis: idx[axis] < sizes[axis] - 1 for axis in AXES}
    barrier = pltpu.get_barrier_semaphore()

    def greet(peer):
        pl.semaphore_signal(barrier, inc=1, device_id=peer, device_id_type=MESH)

    for group in COARSE_GROUPS:
        for_peers(group, sizes, greet)

    def clear(axis, received, ways):
        @pl.when(jnp.logical_not(ways[axis]))
        def _():
            for op in ops:
                for ref in received(op):
                    ref[...] = jnp.zeros_like(ref)

    for j, axis in enumerate(AXES):
        clear(axis, lambda op: op[4 + j : 5 + j], upper)
        clear(axis, lambda op: op[7 + j : 8 + j], lower)

    rows = ops[0][0].shape[1]
    wide = lz * block

    def gate(d, c):
        return pat_ref[0, 0, c : c + 1, d : d + 1].astype(F32)

    def put(ref_h, ref_l, at_rows, at_cols, value):
        high, low = split_pair(value)
        ref_h[at_rows, at_cols] = high
        ref_l[at_rows, at_cols] = low

    def span(c):
        return slice(c * block, (c + 1) * block)

    def halo_copies(k, which=slice(None)):
        field, car_x, car_y, car_z, bey_x, bey_y, bey_z, arr_x, arr_y, arr_z = ops[k]
        routes = (
            ("gx", -1, field, bey_x),
            ("gy", -1, field, bey_y),
            ("gz", -1, field.at[0], bey_z),
            ("gx", 1, car_x, arr_x),
            ("gy", 1, car_y, arr_y),
            ("gz", 1, car_z, arr_z),
        )
        copies = []
        for j, (axis, way, src, dst) in list(enumerate(routes))[which]:
            copies.append(
                (
                    lower[axis] if way < 0 else upper[axis],
                    upper[axis] if way < 0 else lower[axis],
                    pltpu.make_async_remote_copy(
                        src_ref=src,
                        dst_ref=dst,
                        send_sem=halo_send.at[k, j],
                        recv_sem=halo_recv.at[k, j],
                        device_id={axis: jnp.clip(idx[axis] + way, 0, sizes[axis] - 1)},
                        device_id_type=MESH,
                    ),
                )
            )
        return copies

    def start(copies):
        for sends, _, copy in copies:
            pl.when(sends)(copy.start)

    def arrive(copies):
        for _, comes, copy in copies:
            pl.when(comes)(copy.wait_recv)

    def keep(k, v):
        field = ops[k][0]
        for c in range(lz):
            field[c] = v[:, span(c)]

    def carry(k, parts):
        _, car_x, car_y, car_z = ops[k][:4]
        for c in range(lz):
            carried = times(parts[:, span(c)], out_h[c], out_l[c])
            car_x[c] = carried[:, span(0)]
            car_y[c] = carried[:, span(1)]
        car_z[...] = times(parts[:, span(lz - 1)], zo_h[...], zo_l[...])

    def from_above(k):
        bey_x, bey_y, bey_z = ops[k][4:7]
        arrive(halo_copies(k, slice(0, 3)))
        out = []
        for c in range(lz):
            beyond = jnp.concatenate([bey_x[c], bey_y[c]], axis=1)
            part = times(split_rows(beyond), in_h[c], in_l[c])
            if c == lz - 1:
                part = part + times(split_rows(bey_z[...]), zi_h[...], zi_l[...])
            out.append(part)
        return jnp.concatenate(out, axis=1)

    def from_below(k):
        arr_x, arr_y, arr_z = ops[k][7:10]
        arrive(halo_copies(k, slice(3, 6)))
        out = []
        for c in range(lz):
            part = arr_x[c] + arr_y[c]
            if c == 0:
                part = part + arr_z[...]
            out.append(part)
        return jnp.concatenate(out, axis=1)

    def gathered(buf, sem):
        rest = buf.at[pl.ds(0, buf.shape[0] - 1)]
        return pltpu.make_async_copy(rest, rest, sem)

    def reduce_start(buf, group, sem, value):
        me = position(group, sizes)
        buf[me] = value
        own = buf.at[me]

        def send(peer):
            pltpu.make_async_remote_copy(
                src_ref=own,
                dst_ref=own,
                send_sem=red_send.at[sem],
                recv_sem=red_recv.at[sem],
                device_id=peer,
                device_id_type=MESH,
            ).start()

        for_peers(group, sizes, send)

    def reduce_done(buf, sem):
        gathered(buf, red_recv.at[sem]).wait()
        return jnp.sum(buf[...], axis=0)

    def moments_start(j, value):
        reduce_start(moment_bufs[j][0], COARSE_GROUPS[0], j * stages, value)

    def moments_next(j, stage):
        value = reduce_done(moment_bufs[j][stage - 1], j * stages + stage - 1)
        reduce_start(moment_bufs[j][stage], COARSE_GROUPS[stage], j * stages + stage, value)

    def moments_done(j):
        return reduce_done(moment_bufs[j][-1], (j + 1) * stages - 1)

    loads[0].wait()
    loads[4].wait()
    right = jnp.concatenate([right_ref[0, 0, c : c + 1, :] for c in range(lz)], axis=1)
    basis = jnp.concatenate([defl_ref[0, 0, c] for c in range(lz)], axis=1)
    first = jnp.concatenate([basis, right, jnp.zeros((rows - defl - 1, wide), F32)], axis=0)
    keep(0, first)
    first_parts = split_rows(first)
    loads[3].wait()
    loads[2].wait()
    for c in range(lz):
        put(out_h.at[c], out_l.at[c], slice(None), span(0), gate(0, c) * coup_ref[0, 0, 0, c])
        put(out_h.at[c], out_l.at[c], slice(None), span(1), gate(1, c) * coup_ref[1, 0, 0, c])
        if c + 1 == lz:
            put(zo_h, zo_l, slice(None), slice(None), gate(2, c) * coup_ref[2, 0, 0, c])
    carry(0, first_parts)
    pl.semaphore_wait(barrier, sum(extent(group, sizes) - 1 for group in COARSE_GROUPS))
    start(halo_copies(0))

    loads[1].wait()
    square_row = lax.broadcasted_iota(jnp.int32, (block, block), 0)
    square_col = lax.broadcasted_iota(jnp.int32, (block, block), 1)
    shift = jnp.where(square_row == square_col, SHIFT, 0.0)
    if lz > 2:
        loc_h[...] = jnp.zeros_like(loc_h)
        loc_l[...] = jnp.zeros_like(loc_l)
    for c in range(lz):
        put(loc_h, loc_l, span(c), span(c), diag_ref[0, 0, c] - shift)
        cx = gate(0, c) * coup_ref[0, 0, 0, c]
        cy = gate(1, c) * coup_ref[1, 0, 0, c]
        cz = gate(2, c) * coup_ref[2, 0, 0, c]
        put(in_h.at[c], in_l.at[c], span(0), slice(None), cx.T)
        put(in_h.at[c], in_l.at[c], span(1), slice(None), cy.T)
        if c + 1 < lz:
            put(loc_h, loc_l, span(c), span(c + 1), cz)
            put(loc_h, loc_l, span(c + 1), span(c), cz.T)
        else:
            put(zi_h, zi_l, slice(None), slice(None), cz.T)
    row_of = lax.broadcasted_iota(jnp.int32, (rows, wide), 0)
    own = times(first_parts, loc_h[...], loc_l[...]) + jnp.where(row_of < defl, SHIFT * first, 0.0)

    reps = block // defl
    apart = defl // reps
    lane = lax.broadcasted_iota(jnp.int32, (apart, block), 1)
    lane_row = lax.broadcasted_iota(jnp.int32, (1, block), 1)
    col = lax.broadcasted_iota(jnp.int32, (defl, block), 1)
    row = lax.broadcasted_iota(jnp.int32, (defl, block), 0)
    eye = jnp.where(row == col, 1.0, 0.0)

    def project(*below):
        held = sum(v.shape[0] for v in below)
        pads = [jnp.zeros((block - held, wide), F32)]
        put(proj_h, proj_l, slice(None), slice(None), jnp.concatenate([below[0][:defl]] * reps + list(below) + pads, axis=0))

    def pack(repeated):
        packed = jnp.zeros((apart, block), F32)
        for g in range(reps):
            inside = (lane >= g * defl) & (lane < (g + 1) * defl)
            packed = packed + jnp.where(inside, repeated[g * apart : (g + 1) * apart], 0.0)
        return packed

    def unpack(packed):
        groups = [packed] + [pltpu.roll(packed, block - g * defl, 1) for g in range(1, reps)]
        return jnp.where(col < defl, jnp.concatenate(groups, axis=0), 0.0)

    def moments(left, right_parts):
        out_a = times_t(left, proj_h[...], proj_l[...])
        out_b = times_t(right_parts, proj_h[...], proj_l[...])
        vectors = [out[defl : defl + 1, span(1)] for out in (out_a, out_b)]
        return jnp.concatenate([pack(out_a[:defl, span(0)]), pack(out_b[:defl, span(0)])] + vectors, axis=0)

    value = own + from_above(0) + from_below(0)
    chain = [first, value]
    before = first_parts
    for k in range(1, n_ops):
        keep(k, value)
        start(halo_copies(k, slice(0, 3)))
        parts = split_rows(value)
        carry(k, parts)
        start(halo_copies(k, slice(3, 6)))
        if k == 1:
            project(value, first)
        else:
            project(value)
        moments_start(k - 1, moments(before, parts))
        own = times(parts, loc_h[...], loc_l[...])
        for j in range(k - 1):
            stage = k - 1 - j
            if stage < stages:
                moments_next(j, stage)
        if k < ITERS:
            value = own + from_above(k) + from_below(k)
            chain.append(value)
            before = parts
    above = from_above(ITERS)
    half = split_rows((own + 2.0 * above)[:defl])
    peak = pack(times_t(half, proj_h[:block], proj_l[:block]))
    sem = ITERS * stages
    reduce_start(final_bufs[0], final_groups[0], sem, peak)

    e_and_n = moments_done(0)
    coarse = unpack(e_and_n[:apart])
    square = jnp.concatenate([coarse, jnp.zeros((block - defl, block), F32)], axis=0)
    inv = 0.5 * (coarse + square.T[:defl])

    def eliminate(inv, k):
        pivot = 1.0 / inv[k : k + 1, k : k + 1]
        line = jnp.where(col[:1] == k, pivot, inv[k : k + 1] * pivot)
        return jnp.where(row == k, line, jnp.where(col == k, 0.0, inv) - inv[:, k : k + 1] * line)

    pending = [(j, k - j) for k in range(n_ops - 1, n_ops - 1 + stages) for j in range(ITERS) if 0 < k - j < stages and k > n_ops - 2]
    for k in range(defl):
        if k == GJ_FIRST:
            for j, stage in pending:
                moments_next(j, stage)
        inv = eliminate(inv, k)

    lasts = [e_and_n] + [moments_done(j) for j in range(1, ITERS)]
    grams, heads, tails = [], [], []
    for j in range(ITERS):
        packs = [lasts[j][apart : 2 * apart]] if j == 0 else [lasts[j][:apart], lasts[j][apart : 2 * apart]]
        grams += [unpack(p) for p in packs]
        for i in range(2):
            line = lasts[j][2 * apart + i : 2 * apart + i + 1]
            heads.append(jnp.where(lane_row < defl, line, 0.0))
            tails.append(jnp.where(lane_row == defl, line, 0.0))
    start_row = pltpu.roll(lasts[0][2 * apart : 2 * apart + 1], block - rows, 1)
    tails = [jnp.where(lane_row == defl, start_row, 0.0)] + tails
    start_row = jnp.where(lane_row < defl, start_row, 0.0)

    def as_row(c):
        return jnp.sum(eye * c, axis=0, keepdims=True)

    def on(k, c):
        return jnp.sum(grams[k] * c, axis=0, keepdims=True)

    def solve(g):
        return jnp.sum(inv * g, axis=1, keepdims=True)

    def total(line):
        return jnp.sum(line, axis=1, keepdims=True)

    def plus(a, b):
        return b if a is None else a + b

    def spread(c, fields):
        return jnp.sum(c * fields, axis=0, keepdims=True)

    def combine(with_w, with_b, with_h):
        out = None
        if with_w is not None:
            out = spread(with_w, chain[0][:defl])
        for k, c in enumerate(with_b):
            out = plus(out, c * chain[k][defl : defl + 1])
        for k, c in enumerate(with_h):
            out = plus(out, spread(c, chain[k + 1][:defl]))
        return out

    coef = solve(start_row)
    x_w, x_b, x_h = coef, [], []
    rho, rem = [jnp.ones((1, 1), F32)], [-coef]
    dir_w = dir_b = dir_h = curv = norm = None
    for it in range(ITERS):
        deg = it + 1
        rem_rows = [as_row(c) for c in rem]
        grad = None
        for k in range(deg):
            grad = plus(grad, rho[k] * heads[k] + on(k, rem[k]))
        sums = []
        for s in range(2):
            line = None
            for i in range(deg):
                part = None
                for j in range(deg):
                    part = plus(part, 2.0 * rho[j] * heads[i + j + s])
                    line = plus(line, rho[i] * rho[j] * tails[i + j + s])
                if 2 * i + s < len(grams):
                    part = part + on(2 * i + s, rem[i])
                for j in range(i + 1, deg):
                    part = part + 2.0 * on(i + j + s, rem[j])
                line = plus(line, rem_rows[i] * part)
            sums.append(total(line))
        coef = solve(grad)
        energy = total(grad * as_row(coef))
        norm_new = sums[0]
        cross = sums[1] + SHIFT * norm_new
        if it == 0:
            dir_w, dir_b, dir_h = -coef, list(rho), list(rem)
            curv = cross - energy
        else:
            growth = norm_new / norm
            curv = cross - growth * growth * curv - energy
            dir_w = growth * dir_w - coef
            dir_b = [rho[k] + growth * dir_b[k] if k < it else rho[k] for k in range(deg)]
            dir_h = [rem[k] + growth * dir_h[k] if k < it else rem[k] for k in range(deg)]
        norm = norm_new
        img_b = [SHIFT * dir_b[0]] + [dir_b[k - 1] + SHIFT * dir_b[k] for k in range(1, deg)] + [dir_b[-1]]
        img_h = [dir_w + SHIFT * dir_h[0]] + [dir_h[k - 1] + SHIFT * dir_h[k] for k in range(1, deg)] + [dir_h[-1]]
        if it + 1 < ITERS:
            step = norm / curv
            x_w = x_w + step * dir_w
            x_b = [x_b[k] + step * dir_b[k] if k < it else step * dir_b[k] for k in range(deg)]
            x_h = [x_h[k] + step * dir_h[k] if k < it else step * dir_h[k] for k in range(deg)]
            rho = [rho[k] - step * img_b[k] if k < deg else -step * img_b[k] for k in range(deg + 1)]
            rem = [rem[k] - step * img_h[k] if k < deg else -step * img_h[k] for k in range(deg + 1)]
    chain.append(own + above + from_below(ITERS))
    top = rem[-1]
    top_row = as_row(top)
    for g in range(1, reps):
        top_row = top_row + pltpu.roll(as_row(top), g * defl, 1)
    weight = pack(top * top_row)
    x = combine(x_w, x_b, x_h)
    d = combine(dir_w, dir_b, dir_h)
    r = combine(None, rho, rem)
    s = combine(None, img_b, img_h)
    for j in range(1, len(final_groups)):
        peak = reduce_done(final_bufs[j - 1], sem)
        sem += 1
        reduce_start(final_bufs[j], final_groups[j], sem, peak)
    peak = reduce_done(final_bufs[-1], sem)
    curv = curv + total(jnp.sum(peak * weight, axis=0, keepdims=True))
    step = norm / curv
    x = x + step * d
    r = r - step * s
    for c in range(lz):
        sol_ref[0, 0, c : c + 1, :] = x[:, span(c)]
        res_ref[0, 0, c : c + 1, :] = r[:, span(c)]

    for k in range(n_ops):
        for sends, _, copy in halo_copies(k):
            pl.when(sends)(copy.wait_send)
    every = [buf for bufs in moment_bufs for buf in bufs] + list(final_bufs)
    for k, buf in enumerate(every):
        gathered(buf, red_send.at[k]).wait()


def hand_out(sol_ref, res_ref, sol_out, res_out, sol_held, res_held, sems):
    def move(routes, k):
        copies = [pltpu.make_async_copy(src, dst, sems.at[k, j]) for j, (src, dst) in enumerate(routes)]
        for copy in copies:
            copy.start()
        for copy in copies:
            copy.wait()

    move(((sol_ref, sol_held), (res_ref, res_held)), 0)
    move(((sol_held, sol_out), (res_held, res_out)), 1)


def solution(mesh):
    sizes = dict(mesh.shape)
    in_specs = (
        P("gx", "gy", "gz", None),
        P("gx", "gy", "gz", None, None),
        P(None, "gx", "gy", "gz", None, None),
        P(None, "gx", "gy", "gz"),
        P("gx", "gy", "gz", None, None),
    )
    out_specs = (P("gx", "gy", "gz", None), P("gx", "gy", "gz", None))

    def per_device(right_side, diag_blocks, couplings, pattern, deflation):
        lx, ly, lz, block = right_side.shape
        pattern = jnp.transpose(pattern, (1, 2, 3, 0))
        assert lx == 1 and ly == 1
        defl = deflation.shape[3]
        rows_first = (defl + 1 + 7) // 8 * 8
        wide = lz * block
        scratch = []
        for shape in (
            (wide, wide),
            (lz, block, 2 * block),
            (lz, 2 * block, block),
            (block, block),
            (block, block),
            (2 * block, wide),
        ):
            scratch += [pltpu.VMEM(shape, BF16)] * 2
        for _ in range(1 + ITERS):
            layer, face = (lz, rows_first, block), (rows_first, block)
            scratch += [pltpu.VMEM(layer, F32)] * 3 + [pltpu.VMEM(face, F32)]
            scratch += [pltpu.VMEM(layer, F32)] * 2 + [pltpu.VMEM(face, F32)]
            scratch += [pltpu.VMEM(layer, F32)] * 2 + [pltpu.VMEM(face, F32)]
        for _ in range(ITERS):
            for group in COARSE_GROUPS:
                scratch.append(pltpu.VMEM((extent(group, sizes), 2 * defl * defl // block + 2, block), F32))
        for group in last_groups(sizes):
            scratch.append(pltpu.VMEM((extent(group, sizes), defl * defl // block, block), F32))
        reductions = ITERS * len(COARSE_GROUPS) + len(last_groups(sizes))
        scratch += [pltpu.SemaphoreType.DMA((1 + ITERS, 6))] * 2
        scratch += [pltpu.SemaphoreType.DMA((reductions,))] * 2
        scratch.append(pltpu.SemaphoreType.DMA((5,)))
        for array in (right_side, diag_blocks, couplings, pattern, deflation):
            scratch.append(pltpu.VMEM(array.shape, array.dtype))
        vmem = pl.BlockSpec(memory_space=pltpu.VMEM)
        hbm = pl.BlockSpec(memory_space=pltpu.HBM)
        anywhere = pl.BlockSpec(memory_space=pl.ANY)
        out = jax.ShapeDtypeStruct(right_side.shape, F32)
        results = pl.pallas_call(
            functools.partial(kernel, sizes, lz, block, defl),
            out_shape=(out, out),
            in_specs=[hbm] * 5,
            out_specs=(vmem, vmem),
            scratch_shapes=scratch,
            compiler_params=pltpu.CompilerParams(
                collective_id=0, has_side_effects=True, vmem_limit_bytes=67_043_328
            ),
        )(right_side, diag_blocks, couplings, pattern, deflation)
        return pl.pallas_call(
            hand_out,
            out_shape=(out, out),
            in_specs=[anywhere, anywhere],
            out_specs=(hbm, hbm),
            scratch_shapes=[pltpu.VMEM(out.shape, F32)] * 2 + [pltpu.SemaphoreType.DMA((2, 2))],
            compiler_params=pltpu.CompilerParams(vmem_limit_bytes=67_043_328),
        )(*results)

    return jax.shard_map(
        per_device, mesh=mesh, in_specs=in_specs, out_specs=out_specs, check_vma=False
    )
```

```python
import functools
import math

import jax
import jax.numpy as jnp
from jax import lax
from jax.experimental import pallas as pl
from jax.experimental.pallas import tpu as pltpu
from jax.sharding import PartitionSpec as P

ITERS = 3
AXES = ("gx", "gy", "gz")
COARSE_GROUPS = (("gy", "gz"), ("gx",))
UNROLLED = 32
LAST_GROUPS = (("gx", "gy", "gz"),)
DIRECT = 64
SHIFT = 1.45
MESH = pl.DeviceIdType.MESH
F32 = jnp.float32
BF16 = jnp.bfloat16


def place(index, group, sizes):
    coords = {}
    for axis in reversed(group):
        coords[axis] = lax.rem(index, sizes[axis])
        index = lax.div(index, sizes[axis])
    return coords


def position(group, sizes):
    index = 0
    for axis in group:
        index = index * sizes[axis] + lax.axis_index(axis)
    return index


def extent(group, sizes):
    return math.prod(sizes[axis] for axis in group)


def for_peers(group, sizes, action):
    count = extent(group, sizes)
    me = position(group, sizes)

    def body(k, carry):
        action(place(lax.rem(me + k, count), group, sizes))
        return carry

    if count <= UNROLLED:
        for k in range(1, count):
            body(k, 0)
    else:
        lax.fori_loop(1, count, body, 0)


def split_rows(v):
    high = v.astype(BF16).astype(F32)
    rest = v - high
    middle = rest.astype(BF16).astype(F32)
    low = rest - middle
    return jnp.concatenate([high, middle, low], axis=0).astype(BF16)


def join_rows(out, rows):
    return out[:rows] + (out[rows : 2 * rows] + out[2 * rows : 3 * rows])


def split_pair(m):
    high = m.astype(BF16)
    return high, (m - high.astype(F32)).astype(BF16)


def times(parts, high, low):
    out = jnp.dot(parts, high, preferred_element_type=F32)
    out = out + jnp.dot(parts, low, preferred_element_type=F32)
    return join_rows(out, parts.shape[0] // 3)


def times_t(parts, high, low):
    dims = (((1,), (1,)), ((), ()))
    out = lax.dot_general(parts, high, dims, preferred_element_type=F32)
    out = out + lax.dot_general(parts, low, dims, preferred_element_type=F32)
    return join_rows(out, parts.shape[0] // 3)


def last_groups(sizes):
    return LAST_GROUPS if extent(LAST_GROUPS[0], sizes) <= DIRECT else COARSE_GROUPS


def kernel(sizes, lz, block, defl, *refs):
    inputs = refs[:5]
    sol_ref, res_ref = refs[5:7]
    (loc_h, loc_l, out_h, out_l, in_h, in_l, zo_h, zo_l, zi_h, zi_l, proj_h, proj_l) = refs[7:19]
    n_ops = 1 + ITERS
    at = 19
    ops = []
    for _ in range(n_ops):
        ops.append(refs[at : at + 10])
        at += 10
    stages = len(COARSE_GROUPS)
    moment_bufs = [refs[at + j * stages : at + (j + 1) * stages] for j in range(ITERS)]
    at += ITERS * stages
    final_groups = last_groups(sizes)
    final_bufs = refs[at : at + len(final_groups)]
    at += len(final_groups)
    held_ref = refs[at]
    halo_send, halo_recv, red_send, red_recv, load_sem = refs[at + 1 : at + 6]
    staged = refs[at + 6 : at + 11]
    loads = [pltpu.make_async_copy(src, dst, load_sem.at[k]) for k, (src, dst) in enumerate(zip(inputs, staged))]
    for k in (0, 4, 3, 2, 1):
        loads[k].start()
    right_ref, diag_ref, coup_ref, pat_ref, defl_ref = staged

    idx = {axis: lax.axis_index(axis) for axis in AXES}
    lower = {axis: idx[axis] > 0 for axis in AXES}
    upper = {axis: idx[axis] < sizes[axis] - 1 for axis in AXES}
    barrier = pltpu.get_barrier_semaphore()

    def greet(peer):
        pl.semaphore_signal(barrier, inc=1, device_id=peer, device_id_type=MESH)

    for group in COARSE_GROUPS:
        for_peers(group, sizes, greet)

    def clear(axis, received, ways):
        @pl.when(jnp.logical_not(ways[axis]))
        def _():
            for op in ops:
                for ref in received(op):
                    ref[...] = jnp.zeros_like(ref)

    for j, axis in enumerate(AXES):
        clear(axis, lambda op: op[4 + j : 5 + j], upper)
        clear(axis, lambda op: op[7 + j : 8 + j], lower)

    rows = ops[0][0].shape[1]
    wide = lz * block

    def gate(d, c):
        return pat_ref[0, 0, c : c + 1, d : d + 1].astype(F32)

    def put(ref_h, ref_l, at_rows, at_cols, value):
        high, low = split_pair(value)
        ref_h[at_rows, at_cols] = high
        ref_l[at_rows, at_cols] = low

    def span(c):
        return slice(c * block, (c + 1) * block)

    def halo_copies(k, which=slice(None)):
        field, car_x, car_y, car_z, bey_x, bey_y, bey_z, arr_x, arr_y, arr_z = ops[k]
        live = pl.ds(0, defl + 1 if k < ITERS else defl)
        routes = (
            ("gx", -1, field.at[:, live], bey_x.at[:, live]),
            ("gy", -1, field.at[:, live], bey_y.at[:, live]),
            ("gz", -1, field.at[0, live], bey_z.at[live]),
            ("gx", 1, car_x.at[:, live], arr_x.at[:, live]),
            ("gy", 1, car_y.at[:, live], arr_y.at[:, live]),
            ("gz", 1, car_z.at[live], arr_z.at[live]),
        )
        copies = []
        for j, (axis, way, src, dst) in list(enumerate(routes))[which]:
            copies.append(
                (
                    lower[axis] if way < 0 else upper[axis],
                    upper[axis] if way < 0 else lower[axis],
                    pltpu.make_async_remote_copy(
                        src_ref=src,
                        dst_ref=dst,
                        send_sem=halo_send.at[k, j],
                        recv_sem=halo_recv.at[k, j],
                        device_id={axis: jnp.clip(idx[axis] + way, 0, sizes[axis] - 1)},
                        device_id_type=MESH,
                    ),
                )
            )
        return copies

    def start(copies):
        for sends, _, copy in copies:
            pl.when(sends)(copy.start)

    def arrive(copies):
        for _, comes, copy in copies:
            pl.when(comes)(copy.wait_recv)

    def keep(k, v):
        field = ops[k][0]
        for c in range(lz):
            field[c] = v[:, span(c)]

    def carry(k, parts):
        _, car_x, car_y, car_z = ops[k][:4]
        for c in range(lz):
            carried = times(parts[:, span(c)], out_h[c], out_l[c])
            car_x[c] = carried[:, span(0)]
            car_y[c] = carried[:, span(1)]
        car_z[...] = times(parts[:, span(lz - 1)], zo_h[...], zo_l[...])

    def from_above(k):
        bey_x, bey_y, bey_z = ops[k][4:7]
        with jax.named_scope(f"wait_above{k}"):
            arrive(halo_copies(k, slice(0, 3)))
        out = []
        for c in range(lz):
            beyond = jnp.concatenate([bey_x[c], bey_y[c]], axis=1)
            part = times(split_rows(beyond), in_h[c], in_l[c])
            if c == lz - 1:
                part = part + times(split_rows(bey_z[...]), zi_h[...], zi_l[...])
            out.append(part)
        return jnp.concatenate(out, axis=1)

    def from_below(k):
        arr_x, arr_y, arr_z = ops[k][7:10]
        with jax.named_scope(f"wait_below{k}"):
            arrive(halo_copies(k, slice(3, 6)))
        out = []
        for c in range(lz):
            part = arr_x[c] + arr_y[c]
            if c == 0:
                part = part + arr_z[...]
            out.append(part)
        return jnp.concatenate(out, axis=1)

    def gathered(buf, sem):
        rest = buf.at[pl.ds(0, buf.shape[0] - 1)]
        return pltpu.make_async_copy(rest, rest, sem)

    def reduce_start(buf, group, sem, value):
        me = position(group, sizes)
        buf[me] = value
        own = buf.at[me]

        def send(peer):
            pltpu.make_async_remote_copy(
                src_ref=own,
                dst_ref=own,
                send_sem=red_send.at[sem],
                recv_sem=red_recv.at[sem],
                device_id=peer,
                device_id_type=MESH,
            ).start()

        for_peers(group, sizes, send)

    def reduce_done(buf, sem):
        with jax.named_scope(f"wait_sum{sem}"):
            gathered(buf, red_recv.at[sem]).wait()
        return jnp.sum(buf[...], axis=0)

    def spread(c, fields):
        return jnp.sum(c * fields, axis=0, keepdims=True)

    def moments_start(j, value):
        reduce_start(moment_bufs[j][0], COARSE_GROUPS[0], j * stages, value)

    def moments_next(j, stage):
        value = reduce_done(moment_bufs[j][stage - 1], j * stages + stage - 1)
        reduce_start(moment_bufs[j][stage], COARSE_GROUPS[stage], j * stages + stage, value)

    def moments_done(j):
        return reduce_done(moment_bufs[j][-1], (j + 1) * stages - 1)

    with jax.named_scope("load_first"):
        loads[0].wait()
        loads[4].wait()
    right = jnp.concatenate([right_ref[0, 0, c : c + 1, :] for c in range(lz)], axis=1)
    basis = jnp.concatenate([defl_ref[0, 0, c] for c in range(lz)], axis=1)
    first = jnp.concatenate([basis, right, jnp.zeros((rows - defl - 1, wide), F32)], axis=0)
    keep(0, first)
    first_parts = split_rows(first)
    with jax.named_scope("load_second"):
        loads[3].wait()
        loads[2].wait()
    for c in range(lz):
        put(out_h.at[c], out_l.at[c], slice(None), span(0), gate(0, c) * coup_ref[0, 0, 0, c])
        put(out_h.at[c], out_l.at[c], slice(None), span(1), gate(1, c) * coup_ref[1, 0, 0, c])
        if c + 1 == lz:
            put(zo_h, zo_l, slice(None), slice(None), gate(2, c) * coup_ref[2, 0, 0, c])
    with jax.named_scope("barrier"):
        pl.semaphore_wait(barrier, sum(extent(group, sizes) - 1 for group in COARSE_GROUPS))
    start(halo_copies(0, slice(0, 3)))
    with jax.named_scope("carry0"):
        carry(0, first_parts)
    start(halo_copies(0, slice(3, 6)))

    loads[1].wait()
    square_row = lax.broadcasted_iota(jnp.int32, (block, block), 0)
    square_col = lax.broadcasted_iota(jnp.int32, (block, block), 1)
    shift = jnp.where(square_row == square_col, SHIFT, 0.0)
    if lz > 2:
        loc_h[...] = jnp.zeros_like(loc_h)
        loc_l[...] = jnp.zeros_like(loc_l)
    for c in range(lz):
        put(loc_h, loc_l, span(c), span(c), diag_ref[0, 0, c] - shift)
        cx = gate(0, c) * coup_ref[0, 0, 0, c]
        cy = gate(1, c) * coup_ref[1, 0, 0, c]
        cz = gate(2, c) * coup_ref[2, 0, 0, c]
        put(in_h.at[c], in_l.at[c], span(0), slice(None), cx.T)
        put(in_h.at[c], in_l.at[c], span(1), slice(None), cy.T)
        if c + 1 < lz:
            put(loc_h, loc_l, span(c), span(c + 1), cz)
            put(loc_h, loc_l, span(c + 1), span(c), cz.T)
        else:
            put(zi_h, zi_l, slice(None), slice(None), cz.T)
    row_of = lax.broadcasted_iota(jnp.int32, (rows, wide), 0)
    own = times(first_parts, loc_h[...], loc_l[...]) + jnp.where(row_of < defl, SHIFT * first, 0.0)

    reps = block // defl
    apart = defl // reps
    lane = lax.broadcasted_iota(jnp.int32, (apart, block), 1)
    lane_row = lax.broadcasted_iota(jnp.int32, (1, block), 1)
    col = lax.broadcasted_iota(jnp.int32, (defl, block), 1)
    row = lax.broadcasted_iota(jnp.int32, (defl, block), 0)
    eye = jnp.where(row == col, 1.0, 0.0)

    def project(*below):
        held = sum(v.shape[0] for v in below)
        pads = [jnp.zeros((block - held, wide), F32)]
        put(proj_h, proj_l, slice(None), slice(None), jnp.concatenate([below[0][:defl]] * reps + list(below) + pads, axis=0))

    def pack(repeated):
        packed = jnp.zeros((apart, block), F32)
        for g in range(reps):
            inside = (lane >= g * defl) & (lane < (g + 1) * defl)
            packed = packed + jnp.where(inside, repeated[g * apart : (g + 1) * apart], 0.0)
        return packed

    def unpack(packed):
        groups = [packed] + [pltpu.roll(packed, block - g * defl, 1) for g in range(1, reps)]
        return jnp.where(col < defl, jnp.concatenate(groups, axis=0), 0.0)

    def moments(left, right_parts):
        out_a = times_t(left, proj_h[...], proj_l[...])
        out_b = times_t(right_parts, proj_h[...], proj_l[...])
        vectors = [out[defl : defl + 1, span(1)] for out in (out_a, out_b)]
        return jnp.concatenate([pack(out_a[:defl, span(0)]), pack(out_b[:defl, span(0)])] + vectors, axis=0)

    def advance(k, own):
        return jnp.where(row_of <= defl, own + from_above(k) + from_below(k), 0.0)

    value = advance(0, own)
    chain = [first, value]
    before = first_parts
    for k in range(1, n_ops):
        keep(k, value)
        start(halo_copies(k, slice(0, 3)))
        with jax.named_scope(f"carry{k}"):
            parts = split_rows(value)
            carry(k, parts)
        start(halo_copies(k, slice(3, 6)))
        with jax.named_scope(f"moments{k}"):
            if k == 1:
                project(value, first)
            else:
                project(value)
            moments_start(k - 1, moments(before, parts))
        own = times(parts, loc_h[...], loc_l[...])
        for j in range(k - 1):
            stage = k - 1 - j
            if stage < stages:
                moments_next(j, stage)
        if k < ITERS:
            value = advance(k, own)
            chain.append(value)
            before = parts
    pending = [(j, n_ops - 1 - j) for j in range(ITERS) if 0 < n_ops - 1 - j < stages]
    e_and_n = moments_done(0)
    with jax.named_scope("invert"):
        coarse = unpack(e_and_n[:apart])
        square = jnp.concatenate([coarse, jnp.zeros((block - defl, block), F32)], axis=0)
        inv = 0.5 * (coarse + square.T[:defl])

        def eliminate(inv, k):
            col_a, col_b = (jnp.broadcast_to(inv[:, j : j + 1], inv.shape) for j in (k, k + 1))
            a, b, c, d = col_a[k : k + 1], col_b[k : k + 1], col_a[k + 1 : k + 2], col_b[k + 1 : k + 2]
            scale = 1.0 / (a * d - b * c)
            unit_a, unit_b = col[:1] == k, col[:1] == k + 1
            row_a = jnp.where(unit_a, 1.0, jnp.where(unit_b, 0.0, inv[k : k + 1]))
            row_b = jnp.where(unit_b, 1.0, jnp.where(unit_a, 0.0, inv[k + 1 : k + 2]))
            line_a = (d * row_a - b * row_b) * scale
            line_b = (a * row_b - c * row_a) * scale
            rest = jnp.where((col == k) | (col == k + 1), 0.0, inv) - col_a * line_a - col_b * line_b
            return jnp.where(row == k, line_a, jnp.where(row == k + 1, line_b, rest))

        for k in range(0, defl, 2):
            inv = eliminate(inv, k)
        start_row = pltpu.roll(e_and_n[2 * apart : 2 * apart + 1], block - rows, 1)
        first_coef = jnp.sum(inv * jnp.where(lane_row < defl, start_row, 0.0), axis=1, keepdims=True)
        lead = spread(first_coef, chain[ITERS][:defl])
    above = from_above(ITERS)
    with jax.named_scope("peak"):
        peak = lead * spread(first_coef, (own + 2.0 * above)[:defl])
        peak = sum(peak[:, span(c)] for c in range(lz))
        sem = ITERS * stages
        reduce_start(final_bufs[0], final_groups[0], sem, peak)
    for j, stage in pending:
        moments_next(j, stage)

    grams, heads = [], []
    tails = [jnp.where(lane_row == defl, start_row, 0.0)]

    def fetch(j):
        held = e_and_n if j == 0 else moments_done(j)
        packs = [held[apart : 2 * apart]] if j == 0 else [held[:apart], held[apart : 2 * apart]]
        grams.extend(unpack(p) for p in packs)
        for i in range(2):
            line = held[2 * apart + i : 2 * apart + i + 1]
            heads.append(jnp.where(lane_row < defl, line, 0.0))
            tails.append(jnp.where(lane_row == defl, line, 0.0))

    fetch(0)

    def as_row(c):
        return jnp.sum(eye * c, axis=0, keepdims=True)

    def on(k, c):
        return jnp.sum(grams[k] * c, axis=0, keepdims=True)

    def solve(g):
        return jnp.sum(inv * g, axis=1, keepdims=True)

    def total(line):
        return jnp.sum(line, axis=1, keepdims=True)

    def plus(a, b):
        return b if a is None else a + b

    def combine(with_w, with_b, with_h):
        out = None
        if with_w is not None:
            out = spread(with_w, chain[0][:defl])
        for k, c in enumerate(with_b):
            out = plus(out, c * chain[k][defl : defl + 1])
        for k, c in enumerate(with_h):
            out = plus(out, spread(c, chain[k + 1][:defl]))
        return out

    coef = first_coef
    x_w, x_b, x_h = coef, [], []
    rho, rem = [jnp.ones((1, 1), F32)], [-coef]
    scale_top = jnp.ones((1, 1), F32)
    dir_w = dir_b = dir_h = curv = norm = None
    for it in range(ITERS):
        deg = it + 1
        if it + 1 < ITERS:
            fetch(it + 1)
        rem_rows = [as_row(c) for c in rem]
        grad = None
        for k in range(deg):
            grad = plus(grad, rho[k] * heads[k] + on(k, rem[k]))
        sums = []
        for s in range(2):
            line = None
            for i in range(deg):
                part = None
                for j in range(deg):
                    part = plus(part, 2.0 * rho[j] * heads[i + j + s])
                    line = plus(line, rho[i] * rho[j] * tails[i + j + s])
                if 2 * i + s < len(grams):
                    part = part + on(2 * i + s, rem[i])
                for j in range(i + 1, deg):
                    part = part + 2.0 * on(i + j + s, rem[j])
                line = plus(line, rem_rows[i] * part)
            sums.append(total(line))
        coef = solve(grad)
        energy = total(grad * as_row(coef))
        norm_new = sums[0]
        cross = sums[1] + SHIFT * norm_new
        if it == 0:
            dir_w, dir_b, dir_h = -coef, list(rho), list(rem)
            curv = cross - energy
        else:
            growth = norm_new / norm
            curv = cross - growth * growth * curv - energy
            dir_w = growth * dir_w - coef
            dir_b = [rho[k] + growth * dir_b[k] if k < it else rho[k] for k in range(deg)]
            dir_h = [rem[k] + growth * dir_h[k] if k < it else rem[k] for k in range(deg)]
        norm = norm_new
        img_b = [SHIFT * dir_b[0]] + [dir_b[k - 1] + SHIFT * dir_b[k] for k in range(1, deg)] + [dir_b[-1]]
        img_h = [dir_w + SHIFT * dir_h[0]] + [dir_h[k - 1] + SHIFT * dir_h[k] for k in range(1, deg)] + [dir_h[-1]]
        if it + 1 < ITERS:
            step = norm / curv
            scale_top = scale_top * step
            x_w = x_w + step * dir_w
            x_b = [x_b[k] + step * dir_b[k] if k < it else step * dir_b[k] for k in range(deg)]
            x_h = [x_h[k] + step * dir_h[k] if k < it else step * dir_h[k] for k in range(deg)]
            rho = [rho[k] - step * img_b[k] if k < deg else -step * img_b[k] for k in range(deg + 1)]
            rem = [rem[k] - step * img_h[k] if k < deg else -step * img_h[k] for k in range(deg + 1)]
    chain.append(own + above + from_below(ITERS))
    with jax.named_scope("combine"):
        held_ref[0:1] = combine(x_w, x_b, x_h)
        held_ref[1:2] = combine(dir_w, dir_b, dir_h)
        held_ref[2:3] = combine(None, rho, rem)
        held_ref[3:4] = combine(None, img_b, img_h)
    for k in range(n_ops):
        for sends, _, copy in halo_copies(k):
            pl.when(sends)(copy.wait_send)
    every = [buf for bufs in moment_bufs for buf in bufs] + list(final_bufs)
    for k, buf in enumerate(every[:-1]):
        if k < ITERS * stages:
            gathered(buf, red_send.at[k]).wait()
    for j in range(1, len(final_groups)):
        peak = reduce_done(final_bufs[j - 1], sem)
        gathered(final_bufs[j - 1], red_send.at[sem]).wait()
        sem += 1
        reduce_start(final_bufs[j], final_groups[j], sem, peak)
    peak = reduce_done(final_bufs[-1], sem)
    with jax.named_scope("finish"):
        curv = curv + scale_top * scale_top * total(peak)
        step = norm / curv
        x = held_ref[0:1] + step * held_ref[1:2]
        r = held_ref[2:3] - step * held_ref[3:4]
        for c in range(lz):
            sol_ref[0, 0, c : c + 1, :] = x[:, span(c)]
            res_ref[0, 0, c : c + 1, :] = r[:, span(c)]

    gathered(every[-1], red_send.at[len(every) - 1]).wait()


def hand_out(sol_ref, res_ref, sol_out, res_out, sems):
    copies = [pltpu.make_async_copy(sol_ref, sol_out, sems.at[0]), pltpu.make_async_copy(res_ref, res_out, sems.at[1])]
    for copy in copies:
        copy.start()
    for copy in copies:
        copy.wait()


def solution(mesh):
    sizes = dict(mesh.shape)
    in_specs = (
        P("gx", "gy", "gz", None),
        P("gx", "gy", "gz", None, None),
        P(None, "gx", "gy", "gz", None, None),
        P(None, "gx", "gy", "gz"),
        P("gx", "gy", "gz", None, None),
    )
    out_specs = (P("gx", "gy", "gz", None), P("gx", "gy", "gz", None))

    def per_device(right_side, diag_blocks, couplings, pattern, deflation):
        lx, ly, lz, block = right_side.shape
        pattern = jnp.transpose(pattern, (1, 2, 3, 0))
        assert lx == 1 and ly == 1
        defl = deflation.shape[3]
        rows_first = (defl + 1 + 7) // 8 * 8
        wide = lz * block
        scratch = []
        for shape in (
            (wide, wide),
            (lz, block, 2 * block),
            (lz, 2 * block, block),
            (block, block),
            (block, block),
            (2 * block, wide),
        ):
            scratch += [pltpu.VMEM(shape, BF16)] * 2
        for _ in range(1 + ITERS):
            layer, face = (lz, rows_first, block), (rows_first, block)
            scratch += [pltpu.VMEM(layer, F32)] * 3 + [pltpu.VMEM(face, F32)]
            scratch += [pltpu.VMEM(layer, F32)] * 2 + [pltpu.VMEM(face, F32)]
            scratch += [pltpu.VMEM(layer, F32)] * 2 + [pltpu.VMEM(face, F32)]
        for _ in range(ITERS):
            for group in COARSE_GROUPS:
                scratch.append(pltpu.VMEM((extent(group, sizes), 2 * defl * defl // block + 2, block), F32))
        for group in last_groups(sizes):
            scratch.append(pltpu.VMEM((extent(group, sizes), 1, block), F32))
        scratch.append(pltpu.VMEM((8, wide), F32))
        reductions = ITERS * len(COARSE_GROUPS) + len(last_groups(sizes))
        scratch += [pltpu.SemaphoreType.DMA((1 + ITERS, 6))] * 2
        scratch += [pltpu.SemaphoreType.DMA((reductions,))] * 2
        scratch.append(pltpu.SemaphoreType.DMA((5,)))
        for array in (right_side, diag_blocks, couplings, pattern, deflation):
            scratch.append(pltpu.VMEM(array.shape, array.dtype))
        vmem = pl.BlockSpec(memory_space=pltpu.VMEM)
        hbm = pl.BlockSpec(memory_space=pltpu.HBM)
        out = jax.ShapeDtypeStruct(right_side.shape, F32)
        results = pl.pallas_call(
            functools.partial(kernel, sizes, lz, block, defl),
            out_shape=(pltpu.VMEM(out.shape, F32),) * 2,
            in_specs=[hbm] * 5,
            out_specs=(vmem, vmem),
            scratch_shapes=scratch,
            compiler_params=pltpu.CompilerParams(
                collective_id=0, has_side_effects=True, vmem_limit_bytes=67_035_136
            ),
        )(right_side, diag_blocks, couplings, pattern, deflation)
        return pl.pallas_call(
            hand_out,
            out_shape=(out, out),
            in_specs=[vmem, vmem],
            out_specs=(hbm, hbm),
            scratch_shapes=[pltpu.SemaphoreType.DMA((2,))],
            compiler_params=pltpu.CompilerParams(vmem_limit_bytes=1_048_576),
        )(*results)

    return jax.shard_map(
        per_device, mesh=mesh, in_specs=in_specs, out_specs=out_specs, check_vma=False
    )
```

```python
import functools
import math

import jax
import jax.numpy as jnp
from jax import lax
from jax.experimental import pallas as pl
from jax.experimental.pallas import tpu as pltpu
from jax.sharding import PartitionSpec as P

ITERS = 3
AXES = ("gx", "gy", "gz")
COARSE_GROUPS = (("gy", "gz"), ("gx",))
UNROLLED = 32
LAST_GROUPS = (("gx", "gy", "gz"),)
DIRECT = 64
SHIFT = 1.45
MESH = pl.DeviceIdType.MESH
F32 = jnp.float32
BF16 = jnp.bfloat16


def place(index, group, sizes):
    coords = {}
    for axis in reversed(group):
        coords[axis] = lax.rem(index, sizes[axis])
        index = lax.div(index, sizes[axis])
    return coords


def position(group, sizes):
    index = 0
    for axis in group:
        index = index * sizes[axis] + lax.axis_index(axis)
    return index


def extent(group, sizes):
    return math.prod(sizes[axis] for axis in group)


def for_peers(group, sizes, action):
    count = extent(group, sizes)
    me = position(group, sizes)

    def body(k, carry):
        action(place(lax.rem(me + k, count), group, sizes))
        return carry

    if count <= UNROLLED:
        for k in range(1, count):
            body(k, 0)
    else:
        lax.fori_loop(1, count, body, 0)


def split_rows(v):
    high = v.astype(BF16).astype(F32)
    rest = v - high
    middle = rest.astype(BF16).astype(F32)
    low = rest - middle
    return jnp.concatenate([high, middle, low], axis=0).astype(BF16)


def join_rows(out, rows):
    return out[:rows] + (out[rows : 2 * rows] + out[2 * rows : 3 * rows])


def split_pair(m):
    high = m.astype(BF16)
    return high, (m - high.astype(F32)).astype(BF16)


def times(parts, high, low):
    out = jnp.dot(parts, high, preferred_element_type=F32)
    out = out + jnp.dot(parts, low, preferred_element_type=F32)
    return join_rows(out, parts.shape[0] // 3)


def times_t(parts, high, low):
    dims = (((1,), (1,)), ((), ()))
    out = lax.dot_general(parts, high, dims, preferred_element_type=F32)
    out = out + lax.dot_general(parts, low, dims, preferred_element_type=F32)
    return join_rows(out, parts.shape[0] // 3)


def last_groups(sizes):
    return LAST_GROUPS if extent(LAST_GROUPS[0], sizes) <= DIRECT else COARSE_GROUPS


def kernel(sizes, lz, block, defl, *refs):
    inputs = refs[:5]
    sol_ref, res_ref = refs[5:7]
    (loc_h, loc_l, out_h, out_l, in_h, in_l, zo_h, zo_l, zi_h, zi_l, proj_h, proj_l) = refs[7:19]
    n_ops = 1 + ITERS
    at = 19
    ops = []
    for _ in range(n_ops):
        ops.append(refs[at : at + 10])
        at += 10
    stages = len(COARSE_GROUPS)
    moment_bufs = [refs[at + j * stages : at + (j + 1) * stages] for j in range(ITERS)]
    at += ITERS * stages
    final_groups = last_groups(sizes)
    final_bufs = refs[at : at + len(final_groups)]
    at += len(final_groups)
    held_ref = refs[at]
    staged = refs[at + 1 : at + 6]
    halo_send, halo_recv, red_send, red_recv, load_sem = refs[at + 6 : at + 11]
    loads = [pltpu.make_async_copy(src, dst, load_sem.at[k]) for k, (src, dst) in enumerate(zip(inputs, staged))]
    for k in (0, 4, 3, 2, 1):
        loads[k].start()
    right_ref, diag_ref, coup_ref, pat_ref, defl_ref = staged

    idx = {axis: lax.axis_index(axis) for axis in AXES}
    lower = {axis: idx[axis] > 0 for axis in AXES}
    upper = {axis: idx[axis] < sizes[axis] - 1 for axis in AXES}
    barrier = pltpu.get_barrier_semaphore()

    def greet(peer):
        pl.semaphore_signal(barrier, inc=1, device_id=peer, device_id_type=MESH)

    met = 0
    if sizes["gy"] <= 2 and sizes["gx"] <= 4:
        for axis in ("gx", "gy"):
            for there, way in ((lower, -1), (upper, 1)):
                peer = {axis: jnp.clip(idx[axis] + way, 0, sizes[axis] - 1)}
                pl.when(there[axis])(functools.partial(greet, peer))
                met = met + there[axis].astype(jnp.int32)
        for_peers(("gz",), sizes, greet)
        met = met + sizes["gz"] - 1
    else:
        for group in COARSE_GROUPS:
            for_peers(group, sizes, greet)
            met = met + extent(group, sizes) - 1

    def clear(axis, received, ways):
        @pl.when(jnp.logical_not(ways[axis]))
        def _():
            for op in ops:
                for ref in received(op):
                    ref[...] = jnp.zeros_like(ref)

    for j, axis in enumerate(AXES):
        clear(axis, lambda op: op[4 + j : 5 + j], upper)
        clear(axis, lambda op: op[7 + j : 8 + j], lower)

    rows = ops[0][0].shape[1]
    wide = lz * block

    def gate(d, c):
        return pat_ref[0, 0, c : c + 1, d : d + 1].astype(F32)

    def put(ref_h, ref_l, at_rows, at_cols, value):
        high, low = split_pair(value)
        ref_h[at_rows, at_cols] = high
        ref_l[at_rows, at_cols] = low

    def span(c):
        return slice(c * block, (c + 1) * block)

    def halo_copies(k, which=slice(None)):
        field, car_x, car_y, car_z, bey_x, bey_y, bey_z, arr_x, arr_y, arr_z = ops[k]
        live = pl.ds(0, defl + 1 if k < ITERS else defl)
        routes = (
            ("gx", -1, field.at[:, live], bey_x.at[:, live]),
            ("gy", -1, field.at[:, live], bey_y.at[:, live]),
            ("gz", -1, field.at[0, live], bey_z.at[live]),
            ("gx", 1, car_x.at[:, live], arr_x.at[:, live]),
            ("gy", 1, car_y.at[:, live], arr_y.at[:, live]),
            ("gz", 1, car_z.at[live], arr_z.at[live]),
        )
        copies = []
        for j, (axis, way, src, dst) in list(enumerate(routes))[which]:
            copies.append(
                (
                    lower[axis] if way < 0 else upper[axis],
                    upper[axis] if way < 0 else lower[axis],
                    pltpu.make_async_remote_copy(
                        src_ref=src,
                        dst_ref=dst,
                        send_sem=halo_send.at[k, j],
                        recv_sem=halo_recv.at[k, j],
                        device_id={axis: jnp.clip(idx[axis] + way, 0, sizes[axis] - 1)},
                        device_id_type=MESH,
                    ),
                )
            )
        return copies

    def start(copies):
        for sends, _, copy in copies:
            pl.when(sends)(copy.start)

    def arrive(copies):
        for _, comes, copy in copies:
            pl.when(comes)(copy.wait_recv)

    def keep(k, v):
        field = ops[k][0]
        for c in range(lz):
            field[c] = v[:, span(c)]

    def carry(k, parts):
        _, car_x, car_y, car_z = ops[k][:4]
        for c in range(lz):
            carried = times(parts[:, span(c)], out_h[c], out_l[c])
            car_x[c] = carried[:, span(0)]
            car_y[c] = carried[:, span(1)]
        car_z[...] = times(parts[:, span(lz - 1)], zo_h[...], zo_l[...])

    def from_above(k):
        bey_x, bey_y, bey_z = ops[k][4:7]
        with jax.named_scope(f"wait_above{k}"):
            arrive(halo_copies(k, slice(0, 3)))
        out = []
        for c in range(lz):
            beyond = jnp.concatenate([bey_x[c], bey_y[c]], axis=1)
            part = times(split_rows(beyond), in_h[c], in_l[c])
            if c == lz - 1:
                part = part + times(split_rows(bey_z[...]), zi_h[...], zi_l[...])
            out.append(part)
        return jnp.concatenate(out, axis=1)

    def from_below(k):
        arr_x, arr_y, arr_z = ops[k][7:10]
        with jax.named_scope(f"wait_below{k}"):
            arrive(halo_copies(k, slice(3, 6)))
        out = []
        for c in range(lz):
            part = arr_x[c] + arr_y[c]
            if c == 0:
                part = part + arr_z[...]
            out.append(part)
        return jnp.concatenate(out, axis=1)

    def gathered(buf, sem):
        rest = buf.at[pl.ds(0, buf.shape[0] - 1)]
        return pltpu.make_async_copy(rest, rest, sem)

    def reduce_start(buf, group, sem, value):
        me = position(group, sizes)
        buf[me] = value
        own = buf.at[me]

        def send(peer):
            pltpu.make_async_remote_copy(
                src_ref=own,
                dst_ref=own,
                send_sem=red_send.at[sem],
                recv_sem=red_recv.at[sem],
                device_id=peer,
                device_id_type=MESH,
            ).start()

        for_peers(group, sizes, send)

    def reduce_done(buf, sem):
        with jax.named_scope(f"wait_sum{sem}"):
            gathered(buf, red_recv.at[sem]).wait()
        return jnp.sum(buf[...], axis=0)

    def spread(c, fields):
        return jnp.sum(c * fields, axis=0, keepdims=True)

    def moments_start(j, value):
        reduce_start(moment_bufs[j][0], COARSE_GROUPS[0], j * stages, value)

    def moments_next(j, stage):
        value = reduce_done(moment_bufs[j][stage - 1], j * stages + stage - 1)
        reduce_start(moment_bufs[j][stage], COARSE_GROUPS[stage], j * stages + stage, value)

    def moments_done(j):
        return reduce_done(moment_bufs[j][-1], (j + 1) * stages - 1)

    with jax.named_scope("load_first"):
        loads[0].wait()
        loads[4].wait()
    right = jnp.concatenate([right_ref[0, 0, c : c + 1, :] for c in range(lz)], axis=1)
    basis = jnp.concatenate([defl_ref[0, 0, c] for c in range(lz)], axis=1)
    first = jnp.concatenate([basis, right, jnp.zeros((rows - defl - 1, wide), F32)], axis=0)
    keep(0, first)
    first_parts = split_rows(first)
    with jax.named_scope("load_second"):
        loads[3].wait()
        loads[2].wait()
    for c in range(lz):
        put(out_h.at[c], out_l.at[c], slice(None), span(0), gate(0, c) * coup_ref[0, 0, 0, c])
        put(out_h.at[c], out_l.at[c], slice(None), span(1), gate(1, c) * coup_ref[1, 0, 0, c])
        if c + 1 == lz:
            put(zo_h, zo_l, slice(None), slice(None), gate(2, c) * coup_ref[2, 0, 0, c])
    with jax.named_scope("barrier"):
        pl.semaphore_wait(barrier, met)
    start(halo_copies(0, slice(0, 3)))
    with jax.named_scope("carry0"):
        carry(0, first_parts)
    start(halo_copies(0, slice(3, 6)))

    loads[1].wait()
    square_row = lax.broadcasted_iota(jnp.int32, (block, block), 0)
    square_col = lax.broadcasted_iota(jnp.int32, (block, block), 1)
    shift = jnp.where(square_row == square_col, SHIFT, 0.0)
    if lz > 2:
        loc_h[...] = jnp.zeros_like(loc_h)
        loc_l[...] = jnp.zeros_like(loc_l)
    for c in range(lz):
        put(loc_h, loc_l, span(c), span(c), diag_ref[0, 0, c] - shift)
        cx = gate(0, c) * coup_ref[0, 0, 0, c]
        cy = gate(1, c) * coup_ref[1, 0, 0, c]
        cz = gate(2, c) * coup_ref[2, 0, 0, c]
        put(in_h.at[c], in_l.at[c], span(0), slice(None), cx.T)
        put(in_h.at[c], in_l.at[c], span(1), slice(None), cy.T)
        if c + 1 < lz:
            put(loc_h, loc_l, span(c), span(c + 1), cz)
            put(loc_h, loc_l, span(c + 1), span(c), cz.T)
        else:
            put(zi_h, zi_l, slice(None), slice(None), cz.T)
    row_of = lax.broadcasted_iota(jnp.int32, (rows, wide), 0)
    own = times(first_parts, loc_h[...], loc_l[...]) + jnp.where(row_of < defl, SHIFT * first, 0.0)

    reps = block // defl
    apart = defl // reps
    lane = lax.broadcasted_iota(jnp.int32, (apart, block), 1)
    lane_row = lax.broadcasted_iota(jnp.int32, (1, block), 1)
    col = lax.broadcasted_iota(jnp.int32, (defl, block), 1)
    row = lax.broadcasted_iota(jnp.int32, (defl, block), 0)
    eye = jnp.where(row == col, 1.0, 0.0)

    def project(*below):
        held = sum(v.shape[0] for v in below)
        pads = [jnp.zeros((block - held, wide), F32)]
        put(proj_h, proj_l, slice(None), slice(None), jnp.concatenate([below[0][:defl]] * reps + list(below) + pads, axis=0))

    def pack(repeated):
        packed = jnp.zeros((apart, block), F32)
        for g in range(reps):
            inside = (lane >= g * defl) & (lane < (g + 1) * defl)
            packed = packed + jnp.where(inside, repeated[g * apart : (g + 1) * apart], 0.0)
        return packed

    def unpack(packed):
        groups = [packed] + [pltpu.roll(packed, block - g * defl, 1) for g in range(1, reps)]
        return jnp.where(col < defl, jnp.concatenate(groups, axis=0), 0.0)

    def moments(left, right_parts):
        out_a = times_t(left, proj_h[...], proj_l[...])
        out_b = times_t(right_parts, proj_h[...], proj_l[...])
        vectors = [out[defl : defl + 1, span(1)] for out in (out_a, out_b)]
        return jnp.concatenate([pack(out_a[:defl, span(0)]), pack(out_b[:defl, span(0)])] + vectors, axis=0)

    def advance(k, own):
        return jnp.where(row_of <= defl, own + from_above(k) + from_below(k), 0.0)

    value = advance(0, own)
    chain = [first, value]
    before = first_parts
    for k in range(1, n_ops):
        keep(k, value)
        start(halo_copies(k, slice(0, 3)))
        with jax.named_scope(f"carry{k}"):
            parts = split_rows(value)
            carry(k, parts)
        start(halo_copies(k, slice(3, 6)))
        with jax.named_scope(f"moments{k}"):
            if k == 1:
                project(value, first)
            else:
                project(value)
            moments_start(k - 1, moments(before, parts))
        own = times(parts, loc_h[...], loc_l[...])
        for j in range(k - 1):
            stage = k - 1 - j
            if stage < stages:
                moments_next(j, stage)
        if k < ITERS:
            value = advance(k, own)
            chain.append(value)
            before = parts
    pending = [(j, n_ops - 1 - j) for j in range(ITERS) if 0 < n_ops - 1 - j < stages]
    e_and_n = moments_done(0)
    with jax.named_scope("invert"):
        coarse = unpack(e_and_n[:apart])
        square = jnp.concatenate([coarse, jnp.zeros((block - defl, block), F32)], axis=0)
        inv = 0.5 * (coarse + square.T[:defl])

        def eliminate(inv, k):
            col_a, col_b = (jnp.broadcast_to(inv[:, j : j + 1], inv.shape) for j in (k, k + 1))
            a, b, c, d = col_a[k : k + 1], col_b[k : k + 1], col_a[k + 1 : k + 2], col_b[k + 1 : k + 2]
            scale = 1.0 / (a * d - b * c)
            unit_a, unit_b = col[:1] == k, col[:1] == k + 1
            row_a = jnp.where(unit_a, 1.0, jnp.where(unit_b, 0.0, inv[k : k + 1]))
            row_b = jnp.where(unit_b, 1.0, jnp.where(unit_a, 0.0, inv[k + 1 : k + 2]))
            line_a = (d * row_a - b * row_b) * scale
            line_b = (a * row_b - c * row_a) * scale
            rest = jnp.where((col == k) | (col == k + 1), 0.0, inv) - col_a * line_a - col_b * line_b
            return jnp.where(row == k, line_a, jnp.where(row == k + 1, line_b, rest))

        for k in range(0, defl, 2):
            inv = eliminate(inv, k)
        start_row = pltpu.roll(e_and_n[2 * apart : 2 * apart + 1], block - rows, 1)
        first_coef = jnp.sum(inv * jnp.where(lane_row < defl, start_row, 0.0), axis=1, keepdims=True)
        lead = spread(first_coef, chain[ITERS][:defl])
    above = from_above(ITERS)
    with jax.named_scope("peak"):
        peak = lead * spread(first_coef, (own + 2.0 * above)[:defl])
        peak = sum(peak[:, span(c)] for c in range(lz))
        sem = ITERS * stages
        reduce_start(final_bufs[0], final_groups[0], sem, peak)
    for j, stage in pending:
        moments_next(j, stage)

    grams, heads = [], []
    tails = [jnp.where(lane_row == defl, start_row, 0.0)]

    def fetch(j):
        held = e_and_n if j == 0 else moments_done(j)
        packs = [held[apart : 2 * apart]] if j == 0 else [held[:apart], held[apart : 2 * apart]]
        grams.extend(unpack(p) for p in packs)
        for i in range(2):
            line = held[2 * apart + i : 2 * apart + i + 1]
            heads.append(jnp.where(lane_row < defl, line, 0.0))
            tails.append(jnp.where(lane_row == defl, line, 0.0))

    fetch(0)

    def as_row(c):
        return jnp.sum(eye * c, axis=0, keepdims=True)

    def on(k, c):
        return jnp.sum(grams[k] * c, axis=0, keepdims=True)

    def solve(g):
        return jnp.sum(inv * g, axis=1, keepdims=True)

    def total(line):
        return jnp.sum(line, axis=1, keepdims=True)

    def plus(a, b):
        return b if a is None else a + b

    def combine(with_w, with_b, with_h):
        out = None
        if with_w is not None:
            out = spread(with_w, chain[0][:defl])
        for k, c in enumerate(with_b):
            out = plus(out, c * chain[k][defl : defl + 1])
        for k, c in enumerate(with_h):
            out = plus(out, spread(c, chain[k + 1][:defl]))
        return out

    coef = first_coef
    x_w, x_b, x_h = coef, [], []
    rho, rem = [jnp.ones((1, 1), F32)], [-coef]
    scale_top = jnp.ones((1, 1), F32)
    dir_w = dir_b = dir_h = curv = norm = None
    for it in range(ITERS):
        deg = it + 1
        if it + 1 < ITERS:
            fetch(it + 1)
        rem_rows = [as_row(c) for c in rem]
        grad = None
        for k in range(deg):
            grad = plus(grad, rho[k] * heads[k] + on(k, rem[k]))
        sums = []
        for s in range(2):
            line = None
            for i in range(deg):
                part = None
                for j in range(deg):
                    part = plus(part, 2.0 * rho[j] * heads[i + j + s])
                    line = plus(line, rho[i] * rho[j] * tails[i + j + s])
                if 2 * i + s < len(grams):
                    part = part + on(2 * i + s, rem[i])
                for j in range(i + 1, deg):
                    part = part + 2.0 * on(i + j + s, rem[j])
                line = plus(line, rem_rows[i] * part)
            sums.append(total(line))
        coef = solve(grad)
        energy = total(grad * as_row(coef))
        norm_new = sums[0]
        cross = sums[1] + SHIFT * norm_new
        if it == 0:
            dir_w, dir_b, dir_h = -coef, list(rho), list(rem)
            curv = cross - energy
        else:
            growth = norm_new / norm
            curv = cross - growth * growth * curv - energy
            dir_w = growth * dir_w - coef
            dir_b = [rho[k] + growth * dir_b[k] if k < it else rho[k] for k in range(deg)]
            dir_h = [rem[k] + growth * dir_h[k] if k < it else rem[k] for k in range(deg)]
        norm = norm_new
        img_b = [SHIFT * dir_b[0]] + [dir_b[k - 1] + SHIFT * dir_b[k] for k in range(1, deg)] + [dir_b[-1]]
        img_h = [dir_w + SHIFT * dir_h[0]] + [dir_h[k - 1] + SHIFT * dir_h[k] for k in range(1, deg)] + [dir_h[-1]]
        if it + 1 < ITERS:
            step = norm / curv
            scale_top = scale_top * step
            x_w = x_w + step * dir_w
            x_b = [x_b[k] + step * dir_b[k] if k < it else step * dir_b[k] for k in range(deg)]
            x_h = [x_h[k] + step * dir_h[k] if k < it else step * dir_h[k] for k in range(deg)]
            rho = [rho[k] - step * img_b[k] if k < deg else -step * img_b[k] for k in range(deg + 1)]
            rem = [rem[k] - step * img_h[k] if k < deg else -step * img_h[k] for k in range(deg + 1)]
    chain.append(own + above + from_below(ITERS))
    with jax.named_scope("combine"):
        held_ref[0:1] = combine(x_w, x_b, x_h)
        held_ref[1:2] = combine(dir_w, dir_b, dir_h)
        held_ref[2:3] = combine(None, rho, rem)
        held_ref[3:4] = combine(None, img_b, img_h)
    for k in range(n_ops):
        for sends, _, copy in halo_copies(k):
            pl.when(sends)(copy.wait_send)
    every = [buf for bufs in moment_bufs for buf in bufs] + list(final_bufs)
    for k, buf in enumerate(every[:-1]):
        if k < ITERS * stages:
            gathered(buf, red_send.at[k]).wait()
    for j in range(1, len(final_groups)):
        peak = reduce_done(final_bufs[j - 1], sem)
        gathered(final_bufs[j - 1], red_send.at[sem]).wait()
        sem += 1
        reduce_start(final_bufs[j], final_groups[j], sem, peak)
    peak = reduce_done(final_bufs[-1], sem)
    with jax.named_scope("finish"):
        curv = curv + scale_top * scale_top * total(peak)
        step = norm / curv
        x = held_ref[0:1] + step * held_ref[1:2]
        r = held_ref[2:3] - step * held_ref[3:4]
        for c in range(lz):
            sol_ref[0, 0, c : c + 1, :] = x[:, span(c)]
            res_ref[0, 0, c : c + 1, :] = r[:, span(c)]

    gathered(every[-1], red_send.at[len(every) - 1]).wait()


def hand_out(sol_ref, res_ref, sol_out, res_out, sems):
    copies = [pltpu.make_async_copy(sol_ref, sol_out, sems.at[0]), pltpu.make_async_copy(res_ref, res_out, sems.at[1])]
    for copy in copies:
        copy.start()
    for copy in copies:
        copy.wait()


def scoped(body, sems, *refs):
    pl.run_scoped(lambda *held: body(*refs, *held), *sems)


def solution(mesh):
    sizes = dict(mesh.shape)
    in_specs = (
        P("gx", "gy", "gz", None),
        P("gx", "gy", "gz", None, None),
        P(None, "gx", "gy", "gz", None, None),
        P(None, "gx", "gy", "gz"),
        P("gx", "gy", "gz", None, None),
    )
    out_specs = (P("gx", "gy", "gz", None), P("gx", "gy", "gz", None))

    def per_device(right_side, diag_blocks, couplings, pattern, deflation):
        lx, ly, lz, block = right_side.shape
        pattern = jnp.transpose(pattern, (1, 2, 3, 0))
        assert lx == 1 and ly == 1
        defl = deflation.shape[3]
        rows_first = (defl + 1 + 7) // 8 * 8
        wide = lz * block
        scratch = []
        for shape in (
            (wide, wide),
            (lz, block, 2 * block),
            (lz, 2 * block, block),
            (block, block),
            (block, block),
            (2 * block, wide),
        ):
            scratch += [pltpu.VMEM(shape, BF16)] * 2
        for _ in range(1 + ITERS):
            layer, face = (lz, rows_first, block), (rows_first, block)
            scratch += [pltpu.VMEM(layer, F32)] * 3 + [pltpu.VMEM(face, F32)]
            scratch += [pltpu.VMEM(layer, F32)] * 2 + [pltpu.VMEM(face, F32)]
            scratch += [pltpu.VMEM(layer, F32)] * 2 + [pltpu.VMEM(face, F32)]
        for _ in range(ITERS):
            for group in COARSE_GROUPS:
                scratch.append(pltpu.VMEM((extent(group, sizes), 2 * defl * defl // block + 2, block), F32))
        for group in last_groups(sizes):
            scratch.append(pltpu.VMEM((extent(group, sizes), 1, block), F32))
        scratch.append(pltpu.VMEM((8, wide), F32))
        for array in (right_side, diag_blocks, couplings, pattern, deflation):
            scratch.append(pltpu.VMEM(array.shape, array.dtype))
        reductions = ITERS * len(COARSE_GROUPS) + len(last_groups(sizes))
        halo, reds = pltpu.SemaphoreType.DMA((1 + ITERS, 6)), pltpu.SemaphoreType.DMA((reductions,))
        sems = (halo, halo, reds, reds, pltpu.SemaphoreType.DMA((5,)))
        vmem = pl.BlockSpec(memory_space=pltpu.VMEM)
        hbm = pl.BlockSpec(memory_space=pltpu.HBM)
        out = jax.ShapeDtypeStruct(right_side.shape, F32)
        results = pl.pallas_call(
            functools.partial(scoped, functools.partial(kernel, sizes, lz, block, defl), sems),
            out_shape=(pltpu.VMEM(out.shape, F32),) * 2,
            in_specs=[hbm] * 5,
            out_specs=(vmem, vmem),
            scratch_shapes=scratch,
            compiler_params=pltpu.CompilerParams(
                collective_id=0, has_side_effects=True, vmem_limit_bytes=67_035_136
            ),
        )(right_side, diag_blocks, couplings, pattern, deflation)
        return pl.pallas_call(
            hand_out,
            out_shape=(out, out),
            in_specs=[vmem, vmem],
            out_specs=(hbm, hbm),
            scratch_shapes=[pltpu.SemaphoreType.DMA((2,))],
            compiler_params=pltpu.CompilerParams(vmem_limit_bytes=1_048_576),
        )(*results)

    return jax.shard_map(
        per_device, mesh=mesh, in_specs=in_specs, out_specs=out_specs, check_vma=False
    )
```

```python
import functools
import math

import jax
import jax.numpy as jnp
from jax import lax
from jax.experimental import pallas as pl
from jax.experimental.pallas import tpu as pltpu
from jax.sharding import PartitionSpec as P

ITERS = 3
AXES = ("gx", "gy", "gz")
COARSE_GROUPS = (("gy", "gz"), ("gx",))
UNROLLED = 32
LAST_GROUPS = (("gx", "gy", "gz"),)
DIRECT = 64
SHIFT = 1.45
MESH = pl.DeviceIdType.MESH
F32 = jnp.float32
BF16 = jnp.bfloat16


def place(index, group, sizes):
    coords = {}
    for axis in reversed(group):
        coords[axis] = lax.rem(index, sizes[axis])
        index = lax.div(index, sizes[axis])
    return coords


def position(group, sizes):
    index = 0
    for axis in group:
        index = index * sizes[axis] + lax.axis_index(axis)
    return index


def extent(group, sizes):
    return math.prod(sizes[axis] for axis in group)


def for_peers(group, sizes, action):
    count = extent(group, sizes)
    me = position(group, sizes)

    def body(k, carry):
        index = lax.rem(me + k + 1, count)
        action(place(index, group, sizes))
        return carry

    if count <= UNROLLED:
        for k in range(count - 1):
            body(k, 0)
    else:
        lax.fori_loop(0, count - 1, body, 0)


def split_rows(v):
    high = v.astype(BF16).astype(F32)
    rest = v - high
    middle = rest.astype(BF16).astype(F32)
    low = rest - middle
    return jnp.concatenate([high, middle, low], axis=0).astype(BF16)


def join_rows(out, rows):
    return out[:rows] + (out[rows : 2 * rows] + out[2 * rows : 3 * rows])


def split_pair(m):
    high = m.astype(BF16)
    return high, (m - high.astype(F32)).astype(BF16)


def times(parts, *matrices):
    out = jnp.dot(parts, matrices[0], preferred_element_type=F32)
    for matrix in matrices[1:]:
        out = out + jnp.dot(parts, matrix, preferred_element_type=F32)
    return join_rows(out, parts.shape[0] // 3)


def twice(parts):
    return jnp.concatenate([parts, parts], axis=1)


def times_t(parts, high, low):
    dims = (((1,), (1,)), ((), ()))
    out = lax.dot_general(parts, high, dims, preferred_element_type=F32)
    out = out + lax.dot_general(parts, low, dims, preferred_element_type=F32)
    return join_rows(out, parts.shape[0] // 3)


def last_groups(sizes):
    return LAST_GROUPS if extent(LAST_GROUPS[0], sizes) <= DIRECT else COARSE_GROUPS


def kernel(sizes, lz, block, defl, *refs):
    inputs = refs[:5]
    sol_ref, res_ref = refs[5:7]
    loc_h, loc_l, proj_h, proj_l, out_m, in_m, zo_m, zi_m = refs[7:15]
    n_ops = 1 + ITERS
    at = 15
    ops = []
    for _ in range(n_ops):
        ops.append(refs[at : at + 11])
        at += 11
    stages = len(COARSE_GROUPS)
    moment_bufs = [refs[at + j * stages : at + (j + 1) * stages] for j in range(ITERS)]
    at += ITERS * stages
    final_groups = last_groups(sizes)
    final_bufs = refs[at : at + len(final_groups)]
    at += len(final_groups)
    held_ref = refs[at]
    staged = refs[at + 1 : at + 6]
    halo_send, halo_recv, red_send, red_recv, load_sem = refs[at + 6 : at + 11]
    right_ref, diag_ref, coup_ref, pat_ref, defl_ref = staged

    idx = {axis: lax.axis_index(axis) for axis in AXES}
    lower = {axis: idx[axis] > 0 for axis in AXES}
    upper = {axis: idx[axis] < sizes[axis] - 1 for axis in AXES}
    barrier = pltpu.get_barrier_semaphore()

    def greet(peer):
        pl.semaphore_signal(barrier, inc=1, device_id=peer, device_id_type=MESH)

    met = 0
    if sizes["gy"] <= 2 and sizes["gx"] <= 4:
        for axis in ("gx", "gy"):
            for there, way in ((lower, -1), (upper, 1)):
                peer = {axis: jnp.clip(idx[axis] + way, 0, sizes[axis] - 1)}
                pl.when(there[axis])(functools.partial(greet, peer))
                met = met + there[axis].astype(jnp.int32)
        for_peers(("gz",), sizes, greet)
        met = met + sizes["gz"] - 1
    else:
        for group in COARSE_GROUPS:
            for_peers(group, sizes, greet)
            met = met + extent(group, sizes) - 1

    loads = [pltpu.make_async_copy(src, dst, load_sem.at[k]) for k, (src, dst) in enumerate(zip(inputs, staged))]
    for k in (0, 4, 3, 2, 1):
        loads[k].start()

    def clear(axis, received, ways):
        @pl.when(jnp.logical_not(ways[axis]))
        def _():
            for op in ops:
                for ref in received(op):
                    ref[...] = jnp.zeros_like(ref)

    for j, axis in enumerate(AXES):
        clear(axis, lambda op: op[5 + j : 6 + j], upper)
        clear(axis, lambda op: op[8 + j : 9 + j], lower)

    rows = ops[0][1].shape[0]
    wide = lz * block

    def gate(d, c):
        return pat_ref[0, 0, c : c + 1, d : d + 1].astype(F32)

    def put(ref_h, ref_l, at_rows, at_cols, value):
        high, low = split_pair(value)
        ref_h[at_rows, at_cols] = high
        ref_l[at_rows, at_cols] = low

    def span(c):
        return slice(c * block, (c + 1) * block)

    def halo_copies(k, which=slice(None)):
        field, face, car_x, car_y, car_z, bey_x, bey_y, bey_z, arr_x, arr_y, arr_z = ops[k]
        here = defl + 1 if k < ITERS else defl
        layer, edge = pl.ds(0, lz * here), pl.ds(0, here)
        routes = (
            ("gx", -1, field.at[layer], bey_x.at[layer]),
            ("gy", -1, field.at[layer], bey_y.at[layer]),
            ("gz", -1, face.at[edge], bey_z.at[edge]),
            ("gx", 1, car_x.at[layer], arr_x.at[layer]),
            ("gy", 1, car_y.at[layer], arr_y.at[layer]),
            ("gz", 1, car_z.at[edge], arr_z.at[edge]),
        )
        copies = []
        for j, (axis, way, src, dst) in list(enumerate(routes))[which]:
            copies.append(
                (
                    lower[axis] if way < 0 else upper[axis],
                    upper[axis] if way < 0 else lower[axis],
                    pltpu.make_async_remote_copy(
                        src_ref=src,
                        dst_ref=dst,
                        send_sem=halo_send.at[k, j],
                        recv_sem=halo_recv.at[k, j],
                        device_id={axis: jnp.clip(idx[axis] + way, 0, sizes[axis] - 1)},
                        device_id_type=MESH,
                    ),
                )
            )
        return copies

    def start(copies):
        for sends, _, copy in copies:
            pl.when(sends)(copy.start)

    def arrive(copies):
        for _, comes, copy in copies:
            pl.when(comes)(copy.wait_recv)

    def lay(ref, c, v):
        ref[c * defl : (c + 1) * defl] = v[:defl]
        ref[lz * defl + c : lz * defl + c + 1] = v[defl : defl + 1]

    def lift(ref, c):
        tail = jnp.zeros((rows - defl - 1, block), F32)
        parts = [ref[c * defl : (c + 1) * defl], ref[lz * defl + c : lz * defl + c + 1], tail]
        return jnp.concatenate(parts, axis=0)

    def lift_face(ref):
        tail = jnp.zeros((rows - defl - 1, block), F32)
        return jnp.concatenate([ref[:defl], ref[defl : defl + 1], tail], axis=0)

    def keep(k, v):
        field, face = ops[k][:2]
        for c in range(lz):
            lay(field, c, v[:, span(c)])
        face[...] = v[:, span(0)]

    def carry(k, parts):
        car_x, car_y, car_z = ops[k][2:5]
        with jax.named_scope(f"carry{k}"):
            for c in range(lz):
                carried = times(twice(parts[:, span(c)]), out_m[c])
                lay(car_x, c, carried[:, span(0)])
                lay(car_y, c, carried[:, span(1)])
        start(halo_copies(k, slice(3, 5)))
        with jax.named_scope(f"carry_z{k}"):
            car_z[...] = times(twice(parts[:, span(lz - 1)]), zo_m[...])
        start(halo_copies(k, slice(5, 6)))

    def wait_above(k, which):
        with jax.named_scope(f"wait_above{k}"):
            arrive(halo_copies(k, which))

    def above_z(k):
        return times(twice(split_rows(lift_face(ops[k][7]))), zi_m[...])

    def above_xy(k, part_z):
        bey_x, bey_y = ops[k][5:7]
        out = []
        for c in range(lz):
            beyond = jnp.concatenate([lift(bey_x, c), lift(bey_y, c)], axis=1)
            part = times(split_rows(beyond), in_m[c])
            part = part[:, span(0)] + part[:, span(1)]
            out.append(part + part_z if c == lz - 1 else part)
        return jnp.concatenate(out, axis=1)

    def from_below(k):
        arr_x, arr_y, arr_z = ops[k][8:11]
        with jax.named_scope(f"wait_below{k}"):
            arrive(halo_copies(k, slice(3, 6)))
        out = []
        for c in range(lz):
            part = lift(arr_x, c) + lift(arr_y, c)
            if c == 0:
                part = part + lift_face(arr_z)
            out.append(part)
        return jnp.concatenate(out, axis=1)

    def gathered(buf, sem):
        rest = buf.at[pl.ds(0, buf.shape[0] - 1)]
        return pltpu.make_async_copy(rest, rest, sem)

    def reduce_start(buf, group, sem, value):
        me = position(group, sizes)
        buf[me] = value
        own = buf.at[me]

        def send(peer):
            pltpu.make_async_remote_copy(
                src_ref=own,
                dst_ref=own,
                send_sem=red_send.at[sem],
                recv_sem=red_recv.at[sem],
                device_id=peer,
                device_id_type=MESH,
            ).start()

        for_peers(group, sizes, send)

    def reduce_done(buf, sem):
        with jax.named_scope(f"wait_sum{sem}"):
            gathered(buf, red_recv.at[sem]).wait()
        return jnp.sum(buf[...], axis=0)

    def spread(c, fields):
        return jnp.sum(c * fields, axis=0, keepdims=True)

    def moments_start(j, value):
        reduce_start(moment_bufs[j][0], COARSE_GROUPS[0], j * stages, value)

    def moments_next(j, stage):
        value = reduce_done(moment_bufs[j][stage - 1], j * stages + stage - 1)
        reduce_start(moment_bufs[j][stage], COARSE_GROUPS[stage], j * stages + stage, value)

    def moments_done(j):
        return reduce_done(moment_bufs[j][-1], (j + 1) * stages - 1)

    with jax.named_scope("load_first"):
        loads[0].wait()
        loads[4].wait()
    right = jnp.concatenate([right_ref[0, 0, c : c + 1, :] for c in range(lz)], axis=1)
    basis = jnp.concatenate([defl_ref[0, 0, c] for c in range(lz)], axis=1)
    first = jnp.concatenate([basis, right, jnp.zeros((rows - defl - 1, wide), F32)], axis=0)
    keep(0, first)
    first_parts = split_rows(first)
    with jax.named_scope("load_second"):
        loads[3].wait()
        loads[2].wait()
    for c in range(lz):
        for d in range(2):
            high, rest = split_pair(gate(d, c) * coup_ref[d, 0, 0, c])
            out_m[c, span(0), span(d)] = high
            out_m[c, span(1), span(d)] = rest
        if c + 1 == lz:
            high, rest = split_pair(gate(2, c) * coup_ref[2, 0, 0, c])
            zo_m[span(0)] = high
            zo_m[span(1)] = rest
    with jax.named_scope("barrier"):
        pl.semaphore_wait(barrier, met)
    start(halo_copies(0, slice(0, 3)))
    carry(0, first_parts)

    loads[1].wait()
    square_row = lax.broadcasted_iota(jnp.int32, (block, block), 0)
    square_col = lax.broadcasted_iota(jnp.int32, (block, block), 1)
    shift = jnp.where(square_row == square_col, SHIFT, 0.0)
    if lz > 2:
        loc_h[...] = jnp.zeros_like(loc_h)
        loc_l[...] = jnp.zeros_like(loc_l)
    for c in range(lz):
        put(loc_h, loc_l, span(c), span(c), diag_ref[0, 0, c] - shift)
        for d in range(2):
            high, rest = split_pair((gate(d, c) * coup_ref[d, 0, 0, c]).T)
            in_m[c, span(d), span(0)] = high
            in_m[c, span(d), span(1)] = rest
        cz = gate(2, c) * coup_ref[2, 0, 0, c]
        if c + 1 < lz:
            put(loc_h, loc_l, span(c), span(c + 1), cz)
            put(loc_h, loc_l, span(c + 1), span(c), cz.T)
        else:
            high, rest = split_pair(cz.T)
            zi_m[span(0)] = high
            zi_m[span(1)] = rest
    row_of = lax.broadcasted_iota(jnp.int32, (rows, wide), 0)
    own = times(first_parts, loc_h[...], loc_l[...]) + jnp.where(row_of < defl, SHIFT * first, 0.0)

    reps = block // defl
    apart = defl // reps
    lane = lax.broadcasted_iota(jnp.int32, (apart, block), 1)
    lane_row = lax.broadcasted_iota(jnp.int32, (1, block), 1)
    col = lax.broadcasted_iota(jnp.int32, (defl, block), 1)
    row = lax.broadcasted_iota(jnp.int32, (defl, block), 0)
    eye = jnp.where(row == col, 1.0, 0.0)

    def project(*below):
        held = sum(v.shape[0] for v in below)
        pads = [jnp.zeros((block - held, wide), F32)]
        put(proj_h, proj_l, slice(None), slice(None), jnp.concatenate([below[0][:defl]] * reps + list(below) + pads, axis=0))

    def pack(repeated):
        packed = jnp.zeros((apart, block), F32)
        for g in range(reps):
            inside = (lane >= g * defl) & (lane < (g + 1) * defl)
            packed = packed + jnp.where(inside, repeated[g * apart : (g + 1) * apart], 0.0)
        return packed

    def unpack(packed):
        groups = [packed] + [pltpu.roll(packed, block - g * defl, 1) for g in range(1, reps)]
        return jnp.where(col < defl, jnp.concatenate(groups, axis=0), 0.0)

    def moments(left, right_parts):
        out_a = times_t(left, proj_h[...], proj_l[...])
        out_b = times_t(right_parts, proj_h[...], proj_l[...])
        vectors = [out[defl : defl + 1, span(1)] for out in (out_a, out_b)]
        return jnp.concatenate([pack(out_a[:defl, span(0)]), pack(out_b[:defl, span(0)])] + vectors, axis=0)

    def advance(k, own):
        wait_above(k, slice(2, 3))
        part_z = above_z(k)
        wait_above(k, slice(0, 2))
        return own + above_xy(k, part_z) + from_below(k)

    value = advance(0, own)
    chain = [first, value]
    before = first_parts
    for k in range(1, n_ops):
        keep(k, value)
        start(halo_copies(k, slice(0, 3)))
        parts = split_rows(value)

        if k < ITERS:
            carry(k, parts)
        with jax.named_scope(f"moments{k}"):
            project(*((value, first) if k == 1 else (value,)))
            moments_start(k - 1, moments(before, parts))
        if k == ITERS:
            carry(k, parts)
        own = times(parts, loc_h[...], loc_l[...])
        for j in range(k - 1):
            stage = k - 1 - j
            if stage < stages:
                moments_next(j, stage)
        if k < ITERS:
            value = advance(k, own)
            chain.append(value)
            before = parts
    pending = [(j, n_ops - 1 - j) for j in range(ITERS) if 0 < n_ops - 1 - j < stages]
    e_and_n = moments_done(0)
    with jax.named_scope("invert"):
        coarse = unpack(e_and_n[:apart])
        square = jnp.concatenate([coarse, jnp.zeros((block - defl, block), F32)], axis=0)
        inv = 0.5 * (coarse + square.T[:defl])

        def eliminate(inv, k):
            col_a, col_b = (jnp.broadcast_to(inv[:, j : j + 1], inv.shape) for j in (k, k + 1))
            a, b, c, d = col_a[k : k + 1], col_b[k : k + 1], col_a[k + 1 : k + 2], col_b[k + 1 : k + 2]
            scale = 1.0 / (a * d - b * c)
            unit_a, unit_b = col[:1] == k, col[:1] == k + 1
            row_a = jnp.where(unit_a, 1.0, jnp.where(unit_b, 0.0, inv[k : k + 1]))
            row_b = jnp.where(unit_b, 1.0, jnp.where(unit_a, 0.0, inv[k + 1 : k + 2]))
            line_a = (d * row_a - b * row_b) * scale
            line_b = (a * row_b - c * row_a) * scale
            rest = jnp.where((col == k) | (col == k + 1), 0.0, inv) - col_a * line_a - col_b * line_b
            return jnp.where(row == k, line_a, jnp.where(row == k + 1, line_b, rest))

        for k in range(0, defl, 2):
            inv = eliminate(inv, k)
        start_row = pltpu.roll(e_and_n[2 * apart : 2 * apart + 1], block - rows, 1)
        first_coef = jnp.sum(inv * jnp.where(lane_row < defl, start_row, 0.0), axis=1, keepdims=True)
        lead = spread(first_coef, chain[ITERS][:defl])
        inner = lead * spread(first_coef, own[:defl])
        peak_own = sum(inner[:, span(c)] for c in range(lz))
        car_x, car_y, car_z, bey_x, bey_y, bey_z = ops[ITERS][2:8]

        def along(ref, c):
            return spread(first_coef, ref[c * defl : (c + 1) * defl])

        sides = [(bey, c, 2.0 * along(car, c)) for car, bey in ((car_x, bey_x), (car_y, bey_y)) for c in range(lz)]
        sides.append((bey_z, 0, 2.0 * along(car_z, 0)))
    wait_above(ITERS, slice(0, 3))
    with jax.named_scope("peak"):
        peak = peak_own + sum(side * along(bey, c) for bey, c, side in sides)
        sem = ITERS * stages
        reduce_start(final_bufs[0], final_groups[0], sem, peak)
    for j, stage in pending:
        moments_next(j, stage)

    grams, heads = [], []
    tails = [jnp.where(lane_row == defl, start_row, 0.0)]

    def fetch(j):
        held = e_and_n if j == 0 else moments_done(j)
        packs = [held[apart : 2 * apart]] if j == 0 else [held[:apart], held[apart : 2 * apart]]
        grams.extend(unpack(p) for p in packs)
        for i in range(2):
            line = held[2 * apart + i : 2 * apart + i + 1]
            heads.append(jnp.where(lane_row < defl, line, 0.0))
            tails.append(jnp.where(lane_row == defl, line, 0.0))

    fetch(0)

    def as_row(c):
        return jnp.sum(eye * c, axis=0, keepdims=True)

    def on(k, c):
        return jnp.sum(grams[k] * c, axis=0, keepdims=True)

    def solve(g):
        return jnp.sum(inv * g, axis=1, keepdims=True)

    def total(line):
        return jnp.sum(line, axis=1, keepdims=True)

    def plus(a, b):
        return b if a is None else a + b

    def combine(with_w, with_b, with_h):
        out = None
        if with_w is not None:
            out = spread(with_w, chain[0][:defl])
        for k, c in enumerate(with_b):
            out = plus(out, c * chain[k][defl : defl + 1])
        for k, c in enumerate(with_h):
            out = plus(out, spread(c, chain[k + 1][:defl]))
        return out

    coef = first_coef
    x_w, x_b, x_h = coef, [], []
    rho, rem = [jnp.ones((1, 1), F32)], [-coef]
    scale_top = jnp.ones((1, 1), F32)
    dir_w = dir_b = dir_h = curv = norm = None
    for it in range(ITERS):
        deg = it + 1
        if it + 1 < ITERS:
            fetch(it + 1)
        rem_rows = [as_row(c) for c in rem]
        grad = None
        for k in range(deg):
            grad = plus(grad, rho[k] * heads[k] + on(k, rem[k]))
        sums = []
        for s in range(2):
            line = None
            for i in range(deg):
                part = None
                for j in range(deg):
                    part = plus(part, 2.0 * rho[j] * heads[i + j + s])
                    line = plus(line, rho[i] * rho[j] * tails[i + j + s])
                if 2 * i + s < len(grams):
                    part = part + on(2 * i + s, rem[i])
                for j in range(i + 1, deg):
                    part = part + 2.0 * on(i + j + s, rem[j])
                line = plus(line, rem_rows[i] * part)
            sums.append(total(line))
        coef = solve(grad)
        energy = total(grad * as_row(coef))
        norm_new = sums[0]
        cross = sums[1] + SHIFT * norm_new
        if it == 0:
            dir_w, dir_b, dir_h = -coef, list(rho), list(rem)
            curv = cross - energy
        else:
            growth = norm_new / norm
            curv = cross - growth * growth * curv - energy
            dir_w = growth * dir_w - coef
            dir_b = [rho[k] + growth * dir_b[k] if k < it else rho[k] for k in range(deg)]
            dir_h = [rem[k] + growth * dir_h[k] if k < it else rem[k] for k in range(deg)]
        norm = norm_new
        img_b = [SHIFT * dir_b[0]] + [dir_b[k - 1] + SHIFT * dir_b[k] for k in range(1, deg)] + [dir_b[-1]]
        img_h = [dir_w + SHIFT * dir_h[0]] + [dir_h[k - 1] + SHIFT * dir_h[k] for k in range(1, deg)] + [dir_h[-1]]
        if it + 1 < ITERS:
            step = norm / curv
            scale_top = scale_top * step
            x_w = x_w + step * dir_w
            x_b = [x_b[k] + step * dir_b[k] if k < it else step * dir_b[k] for k in range(deg)]
            x_h = [x_h[k] + step * dir_h[k] if k < it else step * dir_h[k] for k in range(deg)]
            rho = [rho[k] - step * img_b[k] if k < deg else -step * img_b[k] for k in range(deg + 1)]
            rem = [rem[k] - step * img_h[k] if k < deg else -step * img_h[k] for k in range(deg + 1)]
    chain.append(own + above_xy(ITERS, above_z(ITERS)) + from_below(ITERS))
    with jax.named_scope("combine"):
        held_ref[0:1] = combine(x_w, x_b, x_h)
        held_ref[1:2] = combine(dir_w, dir_b, dir_h)
        held_ref[2:3] = combine(None, rho, rem)
        held_ref[3:4] = combine(None, img_b, img_h)
    for k in range(n_ops):
        for sends, _, copy in halo_copies(k):
            pl.when(sends)(copy.wait_send)
    every = [buf for bufs in moment_bufs for buf in bufs] + list(final_bufs)
    for k, buf in enumerate(every[:-1]):
        if k < ITERS * stages:
            gathered(buf, red_send.at[k]).wait()
    for j in range(1, len(final_groups)):
        peak = reduce_done(final_bufs[j - 1], sem)
        gathered(final_bufs[j - 1], red_send.at[sem]).wait()
        sem += 1
        reduce_start(final_bufs[j], final_groups[j], sem, peak)
    peak = reduce_done(final_bufs[-1], sem)
    with jax.named_scope("finish"):
        curv = curv + scale_top * scale_top * total(peak)
        step = norm / curv
        x = held_ref[0:1] + step * held_ref[1:2]
        r = held_ref[2:3] - step * held_ref[3:4]
        for c in range(lz):
            sol_ref[0, 0, c : c + 1, :] = x[:, span(c)]
            res_ref[0, 0, c : c + 1, :] = r[:, span(c)]

    gathered(every[-1], red_send.at[len(every) - 1]).wait()


def hand_out(sol_ref, res_ref, sol_out, res_out, sems):
    copies = [pltpu.make_async_copy(sol_ref, sol_out, sems.at[0]), pltpu.make_async_copy(res_ref, res_out, sems.at[1])]
    for copy in copies:
        copy.start()
    for copy in copies:
        copy.wait()


def scoped(body, sems, *refs):
    pl.run_scoped(lambda *held: body(*refs, *held), *sems)


def solution(mesh):
    sizes = dict(mesh.shape)
    in_specs = (
        P("gx", "gy", "gz", None),
        P("gx", "gy", "gz", None, None),
        P(None, "gx", "gy", "gz", None, None),
        P(None, "gx", "gy", "gz"),
        P("gx", "gy", "gz", None, None),
    )
    out_specs = (P("gx", "gy", "gz", None), P("gx", "gy", "gz", None))

    def per_device(right_side, diag_blocks, couplings, pattern, deflation):
        lx, ly, lz, block = right_side.shape
        pattern = jnp.transpose(pattern, (1, 2, 3, 0))
        assert lx == 1 and ly == 1
        defl = deflation.shape[3]
        rows_first = (defl + 1 + 7) // 8 * 8
        wide = lz * block
        scratch = []
        for shape in ((wide, wide), (2 * block, wide)):
            scratch += [pltpu.VMEM(shape, BF16)] * 2
        scratch += [pltpu.VMEM((lz, 2 * block, 2 * block), BF16)] * 2 + [pltpu.VMEM((2 * block, block), BF16)] * 2
        layer, face = ((lz * (defl + 1) + 7) // 8 * 8, block), (rows_first, block)
        for _ in range(1 + ITERS):
            scratch += [pltpu.VMEM(layer, F32), pltpu.VMEM(face, F32)]
            for _ in range(3):
                scratch += [pltpu.VMEM(layer, F32)] * 2 + [pltpu.VMEM(face, F32)]
        for _ in range(ITERS):
            for group in COARSE_GROUPS:
                scratch.append(pltpu.VMEM((extent(group, sizes), 2 * defl * defl // block + 2, block), F32))
        for group in last_groups(sizes):
            scratch.append(pltpu.VMEM((extent(group, sizes), 1, block), F32))
        scratch.append(pltpu.VMEM((8, wide), F32))
        for array in (right_side, diag_blocks, couplings, pattern, deflation):
            scratch.append(pltpu.VMEM(array.shape, array.dtype))
        reductions = ITERS * len(COARSE_GROUPS) + len(last_groups(sizes))
        halo, reds = pltpu.SemaphoreType.DMA((1 + ITERS, 6)), pltpu.SemaphoreType.DMA((reductions,))
        sems = (halo, halo, reds, reds, pltpu.SemaphoreType.DMA((5,)))
        vmem = pl.BlockSpec(memory_space=pltpu.VMEM)
        hbm = pl.BlockSpec(memory_space=pltpu.HBM)
        out = jax.ShapeDtypeStruct(right_side.shape, F32)
        results = pl.pallas_call(
            functools.partial(scoped, functools.partial(kernel, sizes, lz, block, defl), sems),
            out_shape=(pltpu.VMEM(out.shape, F32),) * 2,
            in_specs=[hbm] * 5,
            out_specs=(vmem, vmem),
            scratch_shapes=scratch,
            compiler_params=pltpu.CompilerParams(
                collective_id=0, has_side_effects=True, vmem_limit_bytes=67_035_136
            ),
        )(right_side, diag_blocks, couplings, pattern, deflation)
        return pl.pallas_call(
            hand_out,
            out_shape=(out, out),
            in_specs=[vmem, vmem],
            out_specs=(hbm, hbm),
            scratch_shapes=[pltpu.SemaphoreType.DMA((2,))],
            compiler_params=pltpu.CompilerParams(vmem_limit_bytes=1_048_576),
        )(*results)

    return jax.shard_map(
        per_device, mesh=mesh, in_specs=in_specs, out_specs=out_specs, check_vma=False
    )
```
